128 devices in a mesh: tp: 2 (over core), dpcp: 64 (over z, y, x).
Axes of the slice: x: 4, y: 4, z: 4, core: 2. Of those that a mesh axis runs over, the one named last changes fastest.
Arguments:
- hidden: bfloat16 [128, 512, 576], P('dpcp')
- labels: int32 [128, 512], P('dpcp')
- loss_mask: int32 [128, 512], P('dpcp')
- norm_gain: bfloat16 [576], replicated
- embedding: bfloat16 [49152, 576], P('tp')
Outputs:
- output 1: float32 [], replicated
- output 2: bfloat16 [128, 512, 576], P('dpcp')
- output 3: float32 [49152, 576], P('tp')
All inputs are finite; a program needn't handle non-finite values.
Results may differ from the reference program's by a relative error of at most 0.001.
Values sent between devices are 32-bit elements.
A program may use at most 1 GiB of HBM per device.

```python
import jax
import jax.numpy as jnp
from jax import lax

GROUPS = 64
SEQS_DEV = 2
SEQ = 512
D = 576
V = 49152
BLOCK_ROWS = 16
EPS = 1e-5


def norm_f32(hidden_blk, norm_gain):
    h_f32 = hidden_blk.astype(jnp.float32)
    inv_rms = lax.rsqrt(jnp.mean(h_f32 * h_f32, axis=-1, keepdims=True) + EPS)
    return h_f32 * inv_rms * norm_gain.astype(jnp.float32)


def draw_tokens(key):
    key_lab, key_fill, key_cut, key_end = jax.random.split(key, 4)
    num_rows = GROUPS * SEQS_DEV
    labels = jax.random.randint(key_lab, (num_rows, SEQ), 0, V, jnp.int32)
    labels = labels.at[0, 0].set(0).at[num_rows - 1, SEQ - 1].set(V - 1)
    fill_quarter = jnp.repeat(jax.random.randint(key_fill, (GROUPS,), 1, 5, jnp.int32), SEQS_DEV)
    cut_len = jax.random.randint(key_cut, (num_rows,), 0, SEQ // 8 + 1, jnp.int32)
    seq_lengths = jnp.maximum(SEQ * fill_quarter // 4 - cut_len, 2)[:, None]
    position = jnp.arange(SEQ, dtype=jnp.int32)[None, :]
    doc_end = (jax.random.randint(key_end, (num_rows, SEQ), 0, 8, jnp.int32) == 0) & (position > 0)
    doc_end = doc_end | (position == seq_lengths - 1)
    keep_mask = (position < seq_lengths) & jnp.logical_not(doc_end)
    return labels, keep_mask.astype(jnp.int32)


def setup_inputs(seed: int = 0) -> dict:
    key = jax.random.key(seed)
    key_hid, key_gain, key_emb, key_tok = jax.random.split(key, 4)
    hidden = jax.random.normal(key_hid, (GROUPS * SEQS_DEV, SEQ, D), jnp.float32).astype(jnp.bfloat16)
    norm_gain = (1.0 + 0.3 * jax.random.normal(key_gain, (D,), jnp.float32)).astype(jnp.bfloat16)
    embedding = (jax.random.normal(key_emb, (V, D), jnp.float32) * (2.5 * D ** -0.5)).astype(jnp.bfloat16)
    labels, loss_mask = draw_tokens(key_tok)
    return {"hidden": hidden, "labels": labels, "loss_mask": loss_mask, "norm_gain": norm_gain, "embedding": embedding}


def reference(hidden, labels, loss_mask, norm_gain, embedding):
    num_blocks = GROUPS * SEQS_DEV * SEQ // BLOCK_ROWS
    hid_blocks = hidden.reshape(num_blocks, BLOCK_ROWS, D)
    lab_blocks = labels.reshape(num_blocks, BLOCK_ROWS)
    mask_blocks = loss_mask.reshape(num_blocks, BLOCK_ROWS).astype(jnp.float32)
    mask_count = jnp.sum(mask_blocks)
    vocab_ids = jnp.arange(V, dtype=jnp.int32)[None, :]

    def step(carry, blk_inputs):
        grad_embed, loss_sum = carry
        hid_blk, lab_blk, mask_blk = blk_inputs
        normed_f32, norm_back = jax.vjp(lambda h_in: norm_f32(h_in, norm_gain), hid_blk)
        normed = normed_f32.astype(jnp.bfloat16)
        logits = jnp.dot(normed, embedding.T, preferred_element_type=jnp.float32)
        row_max = jnp.max(logits, axis=-1, keepdims=True)
        exp_vals = jnp.exp(logits - row_max)
        sum_exp = jnp.sum(exp_vals, axis=-1, keepdims=True)
        is_label = vocab_ids == lab_blk[:, None]
        lab_logit = jnp.sum(jnp.where(is_label, logits, 0.0), axis=-1)
        tok_loss = row_max[:, 0] + jnp.log(sum_exp[:, 0]) - lab_logit
        prob_vals = exp_vals / sum_exp
        d_logits = (jnp.where(is_label, prob_vals - 1.0, prob_vals) * (mask_blk / mask_count)[:, None]).astype(jnp.bfloat16)
        d_normed = jnp.dot(d_logits, embedding, preferred_element_type=jnp.float32)
        d_hidden = norm_back(d_normed)[0]
        grad_embed = grad_embed + jnp.dot(d_logits.T, normed, preferred_element_type=jnp.float32)
        return (grad_embed, loss_sum + jnp.sum(mask_blk * tok_loss)), d_hidden

    init_carry = (jnp.zeros((V, D), jnp.float32), jnp.zeros((), jnp.float32))
    (grad_embed, loss_sum), d_blocks = lax.scan(step, init_carry, (hid_blocks, lab_blocks, mask_blocks))
    total_loss = loss_sum / mask_count
    d_hidden = d_blocks.reshape(GROUPS * SEQS_DEV, SEQ, D)
    return (total_loss, d_hidden, grad_embed)
```

```python
import functools

import jax
import jax.numpy as jnp
from jax import lax
from jax.experimental import pallas as pl
from jax.experimental.pallas import tpu as pltpu
from jax.sharding import Mesh
from jax.sharding import PartitionSpec as P

EPS = 1e-5
D = 576
T = 1024
HALF = 512
VSH = 24576
GZ = 4
VZ = VSH // GZ
CHUNKS = (1024, 2048, 2048, 1024)
LANES = 128
NEG = -3.0e38


def dot(a, b):
    return lax.dot_general(a, b, (((1,), (0,)), ((), ())), preferred_element_type=jnp.float32)


def dot_nt(a, b):
    return lax.dot_general(a, b, (((1,), (1,)), ((), ())), preferred_element_type=jnp.float32)


def params(**kw):
    return pltpu.CompilerParams(vmem_limit_bytes=62 * 1024 * 1024, **kw)


def cost(flops, nbytes, trans=0):
    return pl.CostEstimate(flops=int(flops), bytes_accessed=int(nbytes), transcendentals=int(trans))


def norm_kernel(h_ref, g_ref, u_ref, pay_ref):
    h = h_ref[0].astype(jnp.float32)
    inv = lax.rsqrt(jnp.sum(h * h, axis=0, keepdims=True) * (1.0 / D) + EPS)
    n = h * inv * g_ref[...]

    @pl.when(pl.program_id(0) == lax.axis_index("tp"))
    def _():
        pay_ref[...] = n

    u_ref[...] = n.T.astype(jnp.bfloat16)


def norm_call(hid_t, gain):
    return pl.pallas_call(
        norm_kernel,
        grid=(2,),
        in_specs=[
            pl.BlockSpec((1, D, HALF), lambda s: (s, 0, 0)),
            pl.BlockSpec((D, 1), lambda s: (0, 0)),
        ],
        out_specs=[
            pl.BlockSpec((HALF, D), lambda s: (s, 0)),
            pl.BlockSpec((D, HALF), lambda s: (0, 0)),
        ],
        out_shape=[
            jax.ShapeDtypeStruct((T, D), jnp.bfloat16),
            jax.ShapeDtypeStruct((D, HALF), jnp.float32),
        ],
        compiler_params=params(),
        name="norm",
    )(hid_t, gain)


def pack_kernel(own_ref, sib_ref, u_ref, ut_ref):
    me = lax.axis_index("tp")
    for src, half in ((own_ref, me), (sib_ref, 1 - me)):
        n = src[0]
        at = pl.ds(pl.multiple_of(half * HALF, HALF), HALF)
        ut_ref[:, at] = n.astype(jnp.bfloat16)
        u_ref[at, :] = n.T.astype(jnp.bfloat16)


def pack_call(own, sib):
    return pl.pallas_call(
        pack_kernel,
        grid=(GZ,),
        in_specs=[pl.BlockSpec((1, D, HALF), lambda z: (z, 0, 0))] * 2,
        out_specs=[
            pl.BlockSpec((T, D), lambda z: (z, 0)),
            pl.BlockSpec((D, T), lambda z: (0, z)),
        ],
        out_shape=[
            jax.ShapeDtypeStruct((GZ * T, D), jnp.bfloat16),
            jax.ShapeDtypeStruct((D, GZ * T), jnp.bfloat16),
        ],
        compiler_params=params(),
        name="pack",
    )(own, sib)


SVB = 2048
SSUB = 512
SPLIT = 9


def stats_kernel(last, m_in, s_in, u_ref, e_ref, out_ref, s_out, z_scr, m_scr, s_scr):
    @pl.when(pl.program_id(0) == 0)
    def _():
        if last:
            m_scr[...] = m_in[...]
            s_scr[...] = s_in[...]
        else:
            m_scr[...] = jnp.full_like(m_scr, NEG)
            s_scr[...] = jnp.zeros_like(s_scr)

    nsub = SVB // SSUB

    def fold(k):
        for r in range(0, T, 32):
            rows = slice(r, r + 32)
            parts = [z_scr[k, rows, j : j + LANES] for j in range(0, SSUB, LANES)]
            top = functools.reduce(jnp.maximum, parts)
            old = m_scr[rows, :]
            new = jnp.maximum(old, top)
            total = s_scr[rows, :] * jnp.exp(old - new)
            for p in parts:
                total = total + jnp.exp(p - new)
            m_scr[rows, :] = new
            s_scr[rows, :] = total

    for k in range(nsub):
        z_scr[k] = dot(u_ref[...], e_ref[:, k * SSUB : (k + 1) * SSUB])
        if k:
            fold(k - 1)
    fold(nsub - 1)

    @pl.when(pl.program_id(0) == pl.num_programs(0) - 1)
    def _():
        if not last:
            out_ref[...] = m_scr[...]
            s_out[...] = s_scr[...]
            return
        m_lane = m_scr[...]
        m_row = jnp.max(m_lane, axis=1, keepdims=True)
        s_row = jnp.sum(s_scr[...] * jnp.exp(m_lane - m_row), axis=1, keepdims=True)
        out_ref[...] = jnp.broadcast_to(m_row, (T, LANES)).T[0:8, :]
        s_out[...] = jnp.broadcast_to(s_row, (T, LANES)).T[0:8, :]


def stats_call(u, emb_t, before=None):
    total = VSH // SVB
    last = before is not None
    steps, start = (total - SPLIT, SPLIT) if last else (SPLIT, 0)
    shape = (8, T) if last else (T, LANES)
    carried = list(before) if last else []
    kernel = functools.partial(stats_kernel, last)
    if not last:
        kernel = functools.partial(kernel, None, None)
    return pl.pallas_call(
        kernel,
        grid=(steps,),
        in_specs=[pl.BlockSpec((T, LANES), lambda v: (0, 0))] * len(carried)
        + [
            pl.BlockSpec((T, D), lambda v: (0, 0)),
            pl.BlockSpec((D, SVB), lambda v: (0, v + start)),
        ],
        out_specs=[pl.BlockSpec(shape, lambda v: (0, 0))] * 2,
        out_shape=[jax.ShapeDtypeStruct(shape, jnp.float32)] * 2,
        scratch_shapes=[
            pltpu.VMEM((SVB // SSUB, T, SSUB), jnp.float32),
            pltpu.VMEM((T, LANES), jnp.float32),
            pltpu.VMEM((T, LANES), jnp.float32),
        ],
        compiler_params=params(),
        cost_estimate=cost(2 * T * D * SVB * steps, D * SVB * steps * 2, T * SVB * steps),
        name="stats_b" if last else "stats_a",
    )(*carried, u, emb_t)


def spread(row):
    return jnp.broadcast_to(row, (LANES, row.shape[1])).T


def delta_rows(z, row_max, inv_sum, weight, label, ids):
    p = jnp.exp(z - row_max) * inv_sum
    hit = label == ids
    return jnp.where(hit, p - 1.0, p) * weight, hit


def grad_kernel(vb, off, rows_ref, u_ref, ut_ref, e_ref, out_ref, st_scr, z_scr, d_scr):
    xb = pl.program_id(0)

    @pl.when(xb == 0)
    def _():
        for z in range(GZ):
            for k in range(4):
                st_scr[k, z * T : (z + 1) * T, :] = spread(rows_ref[z, k : k + 1, :])

    base = lax.axis_index("tp") * VSH + lax.axis_index("z") * VZ + off + xb * vb
    ids0 = lax.broadcasted_iota(jnp.int32, (32, LANES), 1) + base

    def logits(k, t0):
        z_scr[k] = dot(u_ref[pl.ds(t0, HALF), :], e_ref[...])

    def deltas(k, t0):
        for r in range(0, HALF, 32):
            at = pl.ds(t0 + r, 32)
            row_max, inv_sum, weight, label = (st_scr[i, at, :] for i in range(4))
            for j in range(0, vb, LANES):
                ids = (ids0 + j).astype(jnp.float32)
                d, _ = delta_rows(z_scr[k, r : r + 32, j : j + LANES], row_max, inv_sum, weight, label, ids)
                d_scr[k, r : r + 32, j : j + LANES] = d.astype(jnp.bfloat16)

    out_ref[...] = jnp.zeros_like(out_ref)

    @pl.loop(0, GZ)
    def _(i):
        ta = pl.multiple_of(i * T, T)
        tb = pl.multiple_of(i * T + HALF, HALF)
        logits(0, ta)
        logits(1, tb)
        deltas(0, ta)
        out_ref[:, 0] += dot(ut_ref[:, pl.ds(ta, HALF)], d_scr[0]).reshape(4, D // 4, vb)
        deltas(1, tb)
        out_ref[:, 0] += dot(ut_ref[:, pl.ds(tb, HALF)], d_scr[1]).reshape(4, D // 4, vb)


def grad_call(width, off, rows, u_all, ut_all, emb_t):
    vb = width // 4
    return pl.pallas_call(
        functools.partial(grad_kernel, vb, off),
        grid=(4,),
        in_specs=[
            pl.BlockSpec((GZ, 4, T), lambda x: (0, 0, 0)),
            pl.BlockSpec((GZ * T, D), lambda x: (0, 0), pipeline_mode=pl.Buffered(1)),
            pl.BlockSpec((D, GZ * T), lambda x: (0, 0), pipeline_mode=pl.Buffered(1)),
            pl.BlockSpec((D, vb), lambda x: (0, lax.axis_index("z") * (VZ // vb) + off // vb + x)),
        ],
        out_specs=pl.BlockSpec((4, 1, D // 4, vb), lambda x: (0, x, 0, 0)),
        out_shape=jax.ShapeDtypeStruct((4, 4, D // 4, vb), jnp.float32),
        scratch_shapes=[
            pltpu.VMEM((4, GZ * T, LANES), jnp.float32),
            pltpu.VMEM((2, HALF, vb), jnp.float32),
            pltpu.VMEM((2, HALF, vb), jnp.bfloat16),
        ],
        compiler_params=params(),
        cost_estimate=cost(4 * GZ * T * D * width, D * width * 6 + 4 * GZ * T * D, GZ * T * width),
        name=f"grad{off}",
    )(rows, u_all, ut_all, emb_t)


DVB = 1024
DSUB = 512


def du_kernel(rows_ref, u_ref, e_ref, du_ref, lab_ref, st_scr, z_scr, d_scr, l_scr):
    step = pl.program_id(0)

    @pl.when(step == 0)
    def _():
        for k in range(4):
            st_scr[k] = spread(rows_ref[k : k + 1, :])
        du_ref[...] = jnp.zeros_like(du_ref)
        l_scr[...] = jnp.zeros_like(l_scr)

    base = lax.axis_index("tp") * VSH + step * DVB
    ids0 = lax.broadcasted_iota(jnp.int32, (32, LANES), 1) + base

    def logits(k):
        z_scr[k] = dot(u_ref[...], e_ref[:, k * DSUB : (k + 1) * DSUB])

    def deltas(k):
        for r in range(0, T, 32):
            rows = slice(r, r + 32)
            row_max, inv_sum, weight, label = (st_scr[i, rows, :] for i in range(4))
            found = l_scr[rows, :]
            for j in range(0, DSUB, LANES):
                ids = (ids0 + (k * DSUB + j)).astype(jnp.float32)
                z = z_scr[k, rows, j : j + LANES]
                d, hit = delta_rows(z, row_max, inv_sum, weight, label, ids)
                found = found + jnp.where(hit, z, 0.0)
                d_scr[k, rows, j : j + LANES] = d.astype(jnp.bfloat16)
            l_scr[rows, :] = found

    def product(k):
        du_ref[...] += dot_nt(d_scr[k], e_ref[:, k * DSUB : (k + 1) * DSUB])

    logits(0)
    logits(1)
    deltas(0)
    product(0)
    deltas(1)
    product(1)

    @pl.when(step == pl.num_programs(0) - 1)
    def _():
        lab = jnp.sum(l_scr[...], axis=1, keepdims=True)
        lab_ref[...] = jnp.broadcast_to(lab, (T, LANES)).T[0:8, :]


def du_call(rows, u, emb_t):
    return pl.pallas_call(
        du_kernel,
        grid=(VSH // DVB,),
        in_specs=[
            pl.BlockSpec((4, T), lambda v: (0, 0)),
            pl.BlockSpec((T, D), lambda v: (0, 0)),
            pl.BlockSpec((D, DVB), lambda v: (0, v)),
        ],
        out_specs=[
            pl.BlockSpec((T, D), lambda v: (0, 0)),
            pl.BlockSpec((8, T), lambda v: (0, 0)),
        ],
        out_shape=[
            jax.ShapeDtypeStruct((T, D), jnp.float32),
            jax.ShapeDtypeStruct((8, T), jnp.float32),
        ],
        scratch_shapes=[
            pltpu.VMEM((4, T, LANES), jnp.float32),
            pltpu.VMEM((2, T, DSUB), jnp.float32),
            pltpu.VMEM((2, T, DSUB), jnp.bfloat16),
            pltpu.VMEM((T, LANES), jnp.float32),
        ],
        compiler_params=params(),
        cost_estimate=cost(4 * T * D * VSH, D * VSH * 2, T * VSH),
        name="du",
    )(rows, u, emb_t)


def place_kernel(g_ref, *rest):
    rest[-1][...] = g_ref[0, :, 0].reshape(D, g_ref.shape[-1])


def place_call(width, off, gathered, buf):
    vb = width // 4
    args, specs, alias = [gathered], [], {}
    specs.append(pl.BlockSpec((1, 4, 1, D // 4, vb), lambda z, x: (z, 0, x, 0, 0)))
    if buf is not None:
        args.append(buf)
        specs.append(pl.BlockSpec(memory_space=pl.ANY))
        alias = {1: 0}
    return pl.pallas_call(
        place_kernel,
        grid=(GZ, 4),
        in_specs=specs,
        out_specs=pl.BlockSpec((D, vb), lambda z, x: (0, z * (VZ // vb) + off // vb + x)),
        out_shape=jax.ShapeDtypeStruct((D, VSH), jnp.float32),
        input_output_aliases=alias,
        compiler_params=params(),
        cost_estimate=cost(D * width * 4, D * width * 32),
        name=f"place{off}",
    )(*args)


def norm_f32(hidden_blk, norm_gain):
    h_f32 = hidden_blk.astype(jnp.float32)
    inv_rms = lax.rsqrt(jnp.mean(h_f32 * h_f32, axis=-1, keepdims=True) + EPS)
    return h_f32 * inv_rms * norm_gain.astype(jnp.float32)


def solution(mesh):
    grid_mesh = Mesh(mesh.devices.reshape(2, 4, 4, 4), ("tp", "z", "y", "x"))
    swap = [(0, 1), (1, 0)]

    def local_body(hidden, labels, loss_mask, norm_gain, embedding):
        emb_t = embedding.T
        gain = norm_gain.astype(jnp.float32)[:, None]
        tok_mask = loss_mask.reshape(T).astype(jnp.float32)
        lab = labels.reshape(T).astype(jnp.float32)
        count = lax.psum(jnp.sum(tok_mask), ("tp", "z", "y", "x")) * 0.5
        weight = tok_mask / count

        u, pay = norm_call(hidden.transpose(0, 2, 1), gain)
        own = lax.all_gather(pay, "z", axis=0)
        lanes = stats_call(u, emb_t)
        own, _ = lax.optimization_barrier((own, lanes[0]))
        sib = lax.ppermute(own, "tp", swap)
        m_rows, s_rows = stats_call(u, emb_t, lanes)
        m_loc, s_loc = m_rows[0], s_rows[0]
        row_max = lax.pmax(m_loc, "tp")
        sum_exp = lax.psum(s_loc * jnp.exp(m_loc - row_max), "tp")
        rows = jnp.stack([row_max, 1.0 / sum_exp, weight, lab])
        rows_z = lax.all_gather(rows, "z", axis=0)

        u_all, ut_all = pack_call(own, sib)
        buf = None
        off = 0
        gathered = []
        for width in CHUNKS:
            part = grad_call(width, off, rows_z, u_all, ut_all, emb_t)
            mine = lax.psum_scatter(part.reshape(16, D // 4, width // 4), ("y", "x"), scatter_dimension=0)
            full = lax.all_gather(mine, ("z", "y", "x"), axis=0)
            gathered.append((width, off, full.reshape(GZ, 4, 4, D // 4, width // 4)))
            off += width

        du_part, lab_part = du_call(rows, u, emb_t)
        du = (du_part + lax.ppermute(du_part, "tp", swap)).reshape(2, HALF, D)
        _, norm_back = jax.vjp(lambda h_in: norm_f32(h_in, norm_gain), hidden)
        d_hidden = norm_back(du)[0]

        logs = jnp.where(lax.axis_index("tp") == 0, row_max + jnp.log(sum_exp), 0.0)
        loss = lax.psum(jnp.sum(tok_mask * (logs - lab_part[0])), ("tp", "z", "y", "x")) / count

        for width, off, full in gathered:
            buf = place_call(width, off, full, buf)
        return loss, d_hidden, buf.T

    dp = ("z", "y", "x")
    return jax.shard_map(
        local_body,
        mesh=grid_mesh,
        in_specs=(P(dp, None, None), P(dp, None), P(dp, None), P(None), P("tp", None)),
        out_specs=(P(), P(dp, None, None), P("tp", None)),
        check_vma=False,
    )
```

```python
import functools

import jax
import jax.numpy as jnp
from jax import lax
from jax.experimental import pallas as pl
from jax.experimental.pallas import tpu as pltpu
from jax.sharding import Mesh
from jax.sharding import PartitionSpec as P

EPS = 1e-5
N = {"tp": 2, "z": 4, "y": 4, "x": 4}
D = 576
DP = 640
HALF = 512
T = 2 * HALF
VSH = 24576
VB = 128
SVB, DVB, SUB = 2048, 2048, 512
K = 12
NP = 4
YR = 144
RH = 72
LANES = 128
NEG = -3.0e38
COLORS = (("yzx", (24, 24)), ("xzy", (24, 24)), ("xyz", (24, 24)))
BOTH = ((0, 1), (1, 3))
F32, BF16 = jnp.float32, jnp.bfloat16
FAR = (1, 3, 2)
PAIR, TRIPLE = range(2), range(3)


def mean0(x):
    return jnp.sum(x, axis=0, keepdims=True) * (1.0 / D)


def fold1(op, x):
    return op(x, axis=1, keepdims=True)


def along(axis, *shape):
    return pl.BlockSpec(shape, lambda s: tuple(s if i == axis else 0 for i in range(len(shape))))


def dot(a, b):
    return lax.dot_general(a, b, (((1,), (0,)), ((), ())), preferred_element_type=F32)


def dot_nt(a, b):
    return lax.dot_general(a, b, (((1,), (1,)), ((), ())), preferred_element_type=F32)


def pos(axis, by=0):
    return lax.rem(lax.axis_index(axis) + by, N[axis])


def peers(axis):
    return FAR[: N[axis] - 1]


def whole(shape, **kw):
    return pl.BlockSpec(shape, lambda *_: (0,) * len(shape), **kw)


ANY = pl.BlockSpec(memory_space=pl.ANY)


def push(src, dst, send, recv, axis, by):
    pltpu.make_async_remote_copy(
        src_ref=src,
        dst_ref=dst,
        send_sem=send,
        recv_sem=recv,
        device_id={axis: pos(axis, by)},
        device_id_type=pl.DeviceIdType.MESH,
    ).start()


def wait(ref, sem):
    pltpu.make_async_copy(ref, ref, sem).wait()


def enter():
    barrier = pltpu.get_barrier_semaphore()
    count = 0
    for axis in N:
        for by in peers(axis):
            pl.semaphore_signal(
                barrier, inc=1, device_id={axis: pos(axis, by)}, device_id_type=pl.DeviceIdType.MESH
            )
            count += 1
    pl.semaphore_wait(barrier, count)


def total(step, axes, own, got, send, recv):
    if step > 0:
        acc = own[step - 1]
        for i, _ in enumerate(peers(axes[step - 1])):
            wait(got.at[step - 1, i], recv.at[step - 1, i])
            wait(got.at[step - 1, i], send.at[step - 1, i])
        for i, _ in enumerate(peers(axes[step - 1])):
            acc = acc + got[step - 1, i]
        own[step] = acc
    if step < len(axes):
        for i, by in enumerate(peers(axes[step])):
            push(own.at[step], got.at[step, i], send.at[step, i], recv.at[step, i], axes[step], by)


def params(**kw):
    return pltpu.CompilerParams(vmem_limit_bytes=63 << 20, **kw)


def cost(flops, nbytes):
    return pl.CostEstimate(flops=int(flops), bytes_accessed=int(nbytes), transcendentals=0)


def norm_kernel(h_ref, g_ref, u_ref, ut_ref, pay_ref):
    h = h_ref[0].astype(F32)
    inv = lax.rsqrt(mean0(h * h) + EPS)
    n = h * inv * g_ref[...]

    @pl.when(pl.program_id(0) == lax.axis_index("tp"))
    def _():
        pay_ref[...] = n

    ut_ref[...] = n.astype(BF16)
    u_ref[...] = n.T.astype(BF16)


def norm_call(hid_t, gain):
    return pl.pallas_call(
        norm_kernel,
        grid=(2,),
        in_specs=[along(0, 1, D, HALF), whole((D, 1))],
        out_specs=[
            along(0, HALF, D),
            along(1, D, HALF),
            whole((D, HALF)),
        ],
        out_shape=[
            jax.ShapeDtypeStruct((T, D), BF16),
            jax.ShapeDtypeStruct((D, T), BF16),
            jax.ShapeDtypeStruct((D, HALF), F32),
        ],
        compiler_params=params(),
        name="norm",
    )(hid_t, gain)


def norm_back_kernel(h_ref, g_ref, du_ref, out_ref):
    h = h_ref[0].astype(F32)
    inv = lax.rsqrt(mean0(h * h) + EPS)
    gdu = (du_ref[0] + du_ref[1]).T[:D] * g_ref[...]
    mean = mean0(h * gdu)
    out_ref[0] = (inv * gdu - h * (inv * inv * inv * mean)).astype(BF16)


def norm_back_call(hid_t, gain, du):
    block = along(0, 1, D, HALF)
    return pl.pallas_call(
        norm_back_kernel,
        grid=(2,),
        in_specs=[block, whole((D, 1)), along(1, 2, HALF, DP)],
        out_specs=block,
        out_shape=jax.ShapeDtypeStruct((2, D, HALF), BF16),
        compiler_params=params(),
        name="norm_back",
    )(hid_t, gain, du)


def stats_kernel(
    pay, mask_ref, lab_ref, u_ref, e_ref, z_ref, rows_ref, ug, m_scr, s_scr, own, got, ms, rows_got, *sems
):
    c_send, c_recv, u_send, u_recv, r_send, r_recv = sems
    step, steps = pl.program_id(0), pl.num_programs(0)
    cut = D // 2
    near = ((1, 0), (3, 1))

    def at(index, tick):
        pl.when(step == index)(tick)

    def begin():
        m_scr[...] = jnp.full_like(m_scr, NEG)
        s_scr[...] = jnp.zeros_like(s_scr)
        own[0] = jnp.broadcast_to(jnp.sum(mask_ref[...].astype(F32)), own.shape[1:])
        enter()
        if N["z"] > 1:
            for by, i in near:
                push(pay, ug.at[0, i], u_send.at[0, i], u_recv.at[0, i], "z", by)
        total(0, "xyz", own, got, c_send, c_recv)

    def pass_on():
        if N["z"] > 1:
            for i in PAIR:
                wait(ug.at[0, i], u_recv.at[0, i])
            for by, i in near:
                piece = pl.ds(i * cut, cut)
                push(ug.at[0, i, piece], ug.at[0, 2, piece], u_send.at[0, 2 + i], u_recv.at[0, 2 + i], "z", by)
                if N["tp"] > 1:
                    push(ug.at[0, i], ug.at[1, i], u_send.at[1, i], u_recv.at[1, i], "tp", 1)

    def share_far():
        if N["z"] > 1:
            for i in PAIR:
                wait(ug.at[0, 2, pl.ds(i * cut, cut)], u_recv.at[0, 2 + i])
            if N["tp"] > 1:
                push(ug.at[0, 2], ug.at[1, 2], u_send.at[1, 2], u_recv.at[1, 2], "tp", 1)

    at(0, begin)
    for i in range(1, 4):
        at(i, functools.partial(total, i, "xyz", own, got, c_send, c_recv))
    at(steps * 7 // 12, pass_on)
    at(steps - 1, share_far)

    def fold(k):
        for r in range(0, T, 64):
            rows = slice(r, r + 64)
            parts = [z_ref[rows, j : j + LANES] for j in range(k * SUB, (k + 1) * SUB, LANES)]
            old = m_scr[rows, :]
            new = functools.reduce(jnp.maximum, parts, old)
            acc = s_scr[rows, :] * jnp.exp(old - new)
            for p in parts:
                acc = acc + jnp.exp(p - new)
            m_scr[rows, :] = new
            s_scr[rows, :] = acc

    for k in range(SVB // SUB):
        z_ref[:, k * SUB : (k + 1) * SUB] = dot(u_ref[...], e_ref[:, k * SUB : (k + 1) * SUB])
        if k:
            fold(k - 1)
    fold(SVB // SUB - 1)

    @pl.when(step == steps - 1)
    def _():
        m_lane = m_scr[...]
        m_row = fold1(jnp.max, m_lane)
        s_row = fold1(jnp.sum, s_scr[...] * jnp.exp(m_lane - m_row))
        for i, row in enumerate((m_row, s_row)):
            ms[0, 8 * i : 8 * (i + 1)] = jnp.broadcast_to(row, (T, LANES)).T[:8]
        if N["tp"] > 1:
            push(ms.at[0], ms.at[1], r_send.at[3], r_recv.at[3], "tp", 1)
            wait(ms.at[1], r_recv.at[3])
            wait(ms.at[0], r_send.at[3])
        count = own[3, :1, :1]
        rows_ref[0, 4:8, :] = jnp.broadcast_to(1.0 / count, (4, T))
        swap = lax.axis_index("tp") == 1
        for k in PAIR:
            here = slice(k * HALF, (k + 1) * HALF)
            mask = mask_ref[k : k + 1, :].astype(F32)
            top, whole_sum = ms[0, :1, here], ms[0, 8:9, here]
            if N["tp"] > 1:
                m1, m2 = top, ms[1, :1, here]
                top = jnp.maximum(m1, m2)
                a, b = whole_sum * jnp.exp(m1 - top), ms[1, 8:9, here] * jnp.exp(m2 - top)
                whole_sum = jnp.where(swap, b + a, a + b)
            rows_ref[0, :1, here] = top
            rows_ref[0, 1:2, here] = mask / count / whole_sum
            rows_ref[0, 2:3, here] = jnp.where(mask > 0.0, lab_ref[k : k + 1, :].astype(F32), -1.0)
            rows_ref[0, 3:4, here] = mask * (top + jnp.log(whole_sum))
        rows_got[0] = rows_ref[0]
        for i, by in enumerate(peers("z")):
            push(rows_got.at[0], rows_got.at[1 + i], r_send.at[i], r_recv.at[i], "z", by)
        for i, _ in enumerate(peers("z")):
            wait(rows_got.at[1 + i], r_recv.at[i])
            wait(rows_got.at[0], r_send.at[i])
            rows_ref[1 + i] = rows_got[1 + i]
        if N["z"] > 1:
            for i in PAIR:
                wait(pay, u_send.at[0, i])
                wait(ug.at[0, 2, pl.ds(i * cut, cut)], u_send.at[0, 2 + i])
            if N["tp"] > 1:
                for i in TRIPLE:
                    wait(ug.at[0, i], u_send.at[1, i])
                    wait(ug.at[1, i], u_recv.at[1, i])


def stats_call(pay, mask, lab, u, emb_t):
    dma = pltpu.SemaphoreType.DMA
    return pl.pallas_call(
        stats_kernel,
        grid=(VSH // SVB,),
        in_specs=[
            ANY,
            whole((2, HALF)),
            whole((2, HALF)),
            whole((T, D)),
            along(1, D, SVB),
        ],
        out_specs=[along(1, T, SVB), whole((N["z"], 8, T)), ANY],
        out_shape=[
            jax.ShapeDtypeStruct((T, VSH), F32),
            jax.ShapeDtypeStruct((N["z"], 8, T), F32),
            jax.ShapeDtypeStruct((2, 3, D, HALF), F32),
        ],
        scratch_shapes=[
            pltpu.VMEM((T, LANES), F32),
            pltpu.VMEM((T, LANES), F32),
            pltpu.VMEM((4, 8, LANES), F32),
            pltpu.VMEM((3, 3, 8, LANES), F32),
            pltpu.VMEM((2, 16, T), F32),
            pltpu.VMEM((4, 8, T), F32),
            dma((3, 3)),
            dma((3, 3)),
            dma((2, 4)),
            dma((2, 4)),
            dma((4,)),
            dma((4,)),
        ],
        compiler_params=params(collective_id=1, has_side_effects=True),
        cost_estimate=cost(2 * T * D * VSH, T * VSH * 4),
        name="stats",
    )(pay, mask, lab, u, emb_t)


def pack_kernel(u_ref, ut_ref, own_ref, sib_ref, u_out, ut_out):
    r = pl.program_id(0)

    @pl.when(r == 0)
    def _():
        u_out[...] = u_ref[...]
        ut_out[...] = ut_ref[...]

    @pl.when(r > 0)
    def _():
        me = lax.axis_index("tp")
        for src, half in ((own_ref, me), (sib_ref, 1 - me)):
            n = src[0, 0]
            here = pl.ds(pl.multiple_of(half * HALF, HALF), HALF)
            ut_out[:, here] = n.astype(BF16)
            u_out[here, :] = n.T.astype(BF16)


def pack_call(u, ut, ug):
    piece = [pl.BlockSpec((1, 1, D, HALF), lambda r, c=c: (c, jnp.maximum(r - 1, 0), 0, 0)) for c in PAIR]
    return pl.pallas_call(
        pack_kernel,
        grid=(N["z"],),
        in_specs=[whole((T, D)), whole((D, T)), *piece],
        out_specs=[along(0, T, D), along(1, D, T)],
        out_shape=[
            jax.ShapeDtypeStruct((N["z"] * T, D), BF16),
            jax.ShapeDtypeStruct((D, N["z"] * T), BF16),
        ],
        compiler_params=params(),
        name="pack",
    )(u, ut, ug, ug)


def spread(row):
    return jnp.broadcast_to(row, (LANES, row.shape[1])).T


def main_kernel(rows_ref, u_ref, ut_ref, eg_ref, ed_ref, z_hbm, g, du, loss_ref, *scr):
    (st, zs, ds, p, ra1, ra2, rb1, rb2, sums, s_scr, zb, acc, dd, found, own, got) = scr[:16]
    rs_send, rs_recv, ag_send, ag_recv, l_send, l_recv, d_send, d_recv, local, z_sem = scr[16:]
    slot = pl.program_id(0)
    nx, ny = N["x"], N["y"]
    dus = VSH // DVB
    wg = nx * VB
    quarter = VSH // N["z"]
    parts = tuple(enumerate(("xy", "yx"))) if nx > 1 else ()
    cut = RH // 16 * 8


    def block(part, k, i, half=None):
        two = slice(None) if half is None else pl.ds(2 * half, 2)
        if part == 0:
            return p.at[lax.rem(k, NP), i, two, pl.ds(0, RH)]
        return p.at[lax.rem(k, NP), two, i, pl.ds(RH, RH)]

    def line(part, k, i, half=None):
        rows = (slice(None), pl.ds(0, cut), pl.ds(cut, RH - cut))[0 if half is None else 1 + half]
        return sums.at[lax.rem(k, NP), part, i, rows]

    def rs_push(k, part, stage, src, dst, axis, by):
        push(src, dst, rs_send.at[k, part], rs_recv.at[k, part, stage], axis, by)

    def rb1_at(k, part, half):
        return rb1.at[k, part, pl.ds(half * cut, RH - cut if half else cut)]

    def reduce_start(k):
        for part, (axis, _) in parts:
            for half, by in BOTH:
                rs_push(k, part, 0, block(part, k, pos(axis, 2), half), ra1.at[k, part, half], axis, by)

    def reduce_pass(k):
        for part, (axis, _) in parts:
            wait(ra1.at[k, part], rs_recv.at[k, part, 0])
            for half, by in BOTH:
                block(part, k, pos(axis, by), half)[...] += ra1[k, part, half]
        for part, (axis, _) in parts:
            for half, by in BOTH:
                rs_push(k, part, 1, block(part, k, pos(axis, by)), ra2.at[k, part, half], axis, by)

    def reduce_turn(k):
        for part, (axis, _) in parts:
            wait(ra2.at[k, part], rs_recv.at[k, part, 1])
            sums[lax.rem(k, NP), part] = block(part, k, pos(axis))[...] + ra2[k, part, 0] + ra2[k, part, 1]
        for part, (_, axis) in parts:
            for half, by in BOTH:
                rs_push(k, part, 2, line(part, k, pos(axis, 2), half), rb1_at(k, part, half), axis, by)

    def reduce_pass2(k):
        for part, (_, axis) in parts:
            wait(rb1.at[k, part], rs_recv.at[k, part, 2])
            for half, by in BOTH:
                line(part, k, pos(axis, by), half)[...] += rb1_at(k, part, half)[...]
        for part, (_, axis) in parts:
            for half, by in BOTH:
                rs_push(k, part, 3, line(part, k, pos(axis, by)), rb2.at[k, part, half], axis, by)

    def reduce_end(k):
        if not parts:
            s_scr[k] = p[lax.rem(k, NP), 0, 0]
        for part, (_, axis) in parts:
            wait(rb2.at[k, part], rs_recv.at[k, part, 3])
            s_scr[k, pl.ds(part * RH, RH)] = line(part, k, pos(axis))[...] + rb2[k, part, 0] + rb2[k, part, 1]
            wait(g.at[0, pl.ds(0, RH), pl.ds(0, 15 * VB)], rs_send.at[k, part])
        here = pl.ds(pl.multiple_of(pos("z") * quarter + k * wg + pos("x") * VB, LANES), VB)
        pltpu.make_async_copy(s_scr.at[k], g.at[pos("y"), :, here], local).start()
        wait(s_scr.at[k], local)


    def areas(k, color, phase, v, half=None):
        order, rows = COLORS[color]
        place = {a: pos(a) for a in "xyz"}
        for a in order[:phase]:
            place[a] = None
        place[order[phase]] = v
        row0, n = sum(sum(c[1]) for c in COLORS[:color]), sum(rows)
        if half is not None:
            row0, n = row0 + half * rows[0], rows[half]
        ys = slice(None) if place["y"] is None else pl.ds(place["y"], 1)
        for z in range(N["z"]) if place["z"] is None else (place["z"],):
            col, width = z * quarter + k * wg, wg
            if place["x"] is not None:
                col, width = col + place["x"] * VB, VB
            yield g.at[ys, pl.ds(row0, n), pl.ds(pl.multiple_of(col, LANES), width)]

    def units(color, phase):
        n = 1
        for a in COLORS[color][0][:phase]:
            n *= N[a]
        return n

    def bulk(color, count, part=None):
        rows = COLORS[color][1]
        n = sum(rows) if part is None else rows[part]
        return g.at[0, pl.ds(0, n), pl.ds(0, count * VB)]

    def near(k, c, phase):
        axis = COLORS[c][0][phase]
        if phase > 0:
            far_done(k, c, phase - 1)
        if N[axis] > 1:
            for _, by in BOTH:
                for src in areas(k, c, phase, pos(axis)):
                    push(src, src, ag_send.at[k, c], ag_recv.at[k, c, 2 * phase], axis, by)

    def far(k, c, phase):
        axis = COLORS[c][0][phase]
        if N[axis] > 1:
            wait(bulk(c, 2 * units(c, phase)), ag_recv.at[k, c, 2 * phase])
            for half, by in BOTH:
                for src in areas(k, c, phase, pos(axis, N[axis] - by), half):
                    push(src, src, ag_send.at[k, c], ag_recv.at[k, c, 2 * phase + 1], axis, by)

    def far_done(k, c, phase):
        if N[COLORS[c][0][phase]] > 1:
            wait(bulk(c, units(c, phase)), ag_recv.at[k, c, 2 * phase + 1])

    def gather_end(k, c):
        far_done(k, c, 2)
        count = sum(3 * units(c, i) for i in TRIPLE if N[COLORS[c][0][i]] > 1)
        wait(bulk(c, count), ag_send.at[k, c])

    reduces = (reduce_start, reduce_pass, reduce_turn, reduce_pass2, reduce_end)

    def stage(index, tick, *args):
        since = slot - 1 - index

        @pl.when((since >= 0) & (lax.rem(since, 2) == 0) & (since < 2 * K))
        def _():
            tick(since // 2, *args)

    def fetch(i):
        pltpu.make_async_copy(z_hbm.at[:, pl.ds(pl.multiple_of(i * DVB, LANES), DVB)], zb, z_sem).start()

    @pl.when(slot == 0)
    def _():
        fetch(0)
        for r in range(N["z"]):
            for k in TRIPLE:
                st[k, r * T : (r + 1) * T, :] = spread(rows_ref[r, k : k + 1, :])
        acc[...] = jnp.zeros_like(acc)
        found[...] = jnp.zeros_like(found)
        enter()

    for i, tick in enumerate(reduces):
        stage(i, tick)
    for c in range(len(COLORS)):
        for phase in TRIPLE:
            stage(len(reduces) + 2 * phase, near, c, phase)
            stage(len(reduces) + 2 * phase + 1, far, c, phase)
        stage(len(reduces) + 6, gather_end, c)

    hit_value = rows_ref[0, 4:5, :LANES]

    @pl.when((slot < 2 * K) & (lax.rem(slot, 2) == 0))
    def _():
        k = slot // 2
        buf = lax.rem(k, NP)
        base = lax.axis_index("tp") * VSH + lax.axis_index("z") * quarter + k * wg
        ids = (lax.broadcasted_iota(jnp.int32, (16, wg), 1) + base).astype(F32)
        hit_row = jnp.concatenate([hit_value] * nx, axis=1)

        def logits(h, t0):
            zs[h] = dot(u_ref[pl.ds(t0, HALF), :], eg_ref[...])

        def deltas(h, t0):
            for r in range(0, HALF, 16):
                here = pl.ds(t0 + r, 16)
                top, scale, label = (jnp.concatenate([st[i, here, :]] * nx, axis=1) for i in TRIPLE)
                e = jnp.exp(zs[h, r : r + 16, :] - top) * scale
                ds[h, r : r + 16, :] = jnp.where(label == ids, e - hit_row, e).astype(BF16)

        def product(h, t0):
            part = dot(ut_ref[:, pl.ds(t0, HALF)], ds[h]).reshape(ny, YR, wg)
            for i in range(nx):
                p[buf, i] += part[:, :, i * VB : (i + 1) * VB]

        p[buf] = jnp.zeros(p.shape[1:], F32)

        @pl.loop(0, N["z"])
        def _(r):
            ta = pl.multiple_of(r * T, T)
            tb = pl.multiple_of(r * T + HALF, HALF)
            logits(0, ta)
            logits(1, tb)
            deltas(0, ta)
            product(0, ta)
            deltas(1, tb)
            product(1, tb)

    @pl.when((slot < 2 * dus) & (lax.rem(slot, 2) == 1))
    def _():
        i = slot // 2
        wait(zb, z_sem)
        base = lax.axis_index("tp") * VSH + i * DVB
        ids0 = lax.broadcasted_iota(jnp.int32, (32, LANES), 1) + base
        for k in range(DVB // SUB):
            cols = slice(k * SUB, (k + 1) * SUB)
            ids = [(ids0 + j).astype(F32) for j in range(k * SUB, (k + 1) * SUB, LANES)]
            for r in range(0, T, 32):
                here = slice(r, r + 32)
                top, scale, label = (st[n, here, :] for n in TRIPLE)
                hits = found[here, :]
                for j, idj in enumerate(ids):
                    z = zb[here, k * SUB + j * LANES : k * SUB + (j + 1) * LANES]
                    e = jnp.exp(z - top) * scale
                    hit = label == idj
                    hits = hits + jnp.where(hit, z, 0.0)
                    dd[k % 2, here, j * LANES : (j + 1) * LANES] = jnp.where(hit, e - hit_value, e).astype(BF16)
                found[here, :] = hits
            acc[:, :D] += dot_nt(dd[k % 2], ed_ref[:, cols])

        @pl.when(i + 1 < dus)
        def _():
            fetch(i + 1)


    def finish_du():
        if N["tp"] > 1:
            push(acc, du.at[1], d_send.at[0], d_recv, "tp", 1)
        pltpu.make_async_copy(acc, du.at[0], d_send.at[1]).start()
        logs = jnp.where(lax.axis_index("tp") == 0, jnp.sum(rows_ref[0, 3:4, :]), 0.0)
        own[0] = jnp.broadcast_to(logs - jnp.sum(found[...]), own.shape[1:])

    def finish():
        wait(acc, d_send.at[1])
        if N["tp"] > 1:
            wait(acc, d_send.at[0])
            wait(acc, d_recv)
        loss_ref[...] = own[len(AXES)] * hit_value

    pl.when(slot == 2 * dus)(finish_du)
    for i in range(len(AXES) + 1):
        pl.when(slot == 2 * dus + 1 + i)(functools.partial(total, i, AXES, own, got, l_send, l_recv))
    pl.when(slot == pl.num_programs(0) - 1)(finish)


AXES = ("tp", "x", "y", "z")


def main_call(rows, u_all, ut_all, emb_t, logits):
    nx, ny, nz = N["x"], N["y"], N["z"]
    wg = nx * VB
    dus = VSH // DVB
    dma = pltpu.SemaphoreType.DMA

    def grad_block(s):
        return 0, lax.axis_index("z") * K + jnp.minimum(s // 2, K - 1)

    def du_block(s):
        return 0, jnp.minimum(s // 2, dus - 1)

    once = dict(pipeline_mode=pl.Buffered(1))
    return pl.pallas_call(
        main_kernel,
        grid=(2 * K + 12,),
        in_specs=[
            whole((nz, 8, T), **once),
            whole((nz * T, D), **once),
            whole((D, nz * T), **once),
            pl.BlockSpec((D, wg), grad_block),
            pl.BlockSpec((D, DVB), du_block),
            ANY,
        ],
        out_specs=[ANY, ANY, whole((8, LANES))],
        out_shape=[
            jax.ShapeDtypeStruct((ny, YR, VSH), F32),
            jax.ShapeDtypeStruct((2, T, DP), F32),
            jax.ShapeDtypeStruct((8, LANES), F32),
        ],
        scratch_shapes=[
            pltpu.VMEM(shape, F32)
            for shape in (
                (3, nz * T, LANES),
                (2, HALF, wg),
            )
        ]
        + [pltpu.VMEM((2, HALF, wg), BF16)]
        + [
            pltpu.VMEM(shape, F32)
            for shape in (
                (NP, nx, ny, YR, VB),
                (K, 2, 2, 2, RH, VB),
                (K, 2, 2, 4, RH, VB),
                (K, 2, RH, VB),
                (K, 2, 2, RH, VB),
                (NP, 2, 4, RH, VB),
                (K, YR, VB),
                (T, DVB),
                (T, DP),
            )
        ]
        + [
            pltpu.VMEM((2, T, SUB), BF16),
            pltpu.VMEM((T, LANES), F32),
            pltpu.VMEM((5, 8, LANES), F32),
            pltpu.VMEM((4, 3, 8, LANES), F32),
            dma((K, 2)),
            dma((K, 2, 4)),
            dma((K, 3)),
            dma((K, 3, 6)),
            dma((4, 3)),
            dma((4, 3)),
            dma((2,)),
            dma,
            dma,
            dma,
        ],
        compiler_params=params(collective_id=2, has_side_effects=True),
        cost_estimate=cost(6 * T * D * VSH, T * VSH * 4),
        name="main",
    )(rows, u_all, ut_all, emb_t, emb_t, logits)


def solution(mesh):
    axes = tuple(N)
    grid_mesh = Mesh(mesh.devices.reshape(tuple(N.values())), axes)

    def local_body(hidden, labels, loss_mask, norm_gain, embedding):
        emb_t = embedding.T
        hid_t = hidden.transpose(0, 2, 1)
        gain = norm_gain.astype(F32)[:, None]
        u, ut, pay = norm_call(hid_t, gain)
        logits, rows, ug = stats_call(pay, loss_mask, labels, u, emb_t)
        u_all, ut_all = pack_call(u, ut, ug)
        grad, du, loss = main_call(rows, u_all, ut_all, emb_t, logits)
        d_hidden = norm_back_call(hid_t, gain, du)
        return loss[0, 0], d_hidden.transpose(0, 2, 1), grad.reshape(D, VSH).T

    dp = axes[1:]
    return jax.shard_map(
        local_body,
        mesh=grid_mesh,
        in_specs=(P(dp), P(dp), P(dp), P(), P("tp")),
        out_specs=(P(), P(dp), P("tp")),
        check_vma=False,
    )
```

```python
import functools

import jax
import jax.numpy as jnp
from jax import lax
from jax.experimental import pallas as pl
from jax.experimental.pallas import tpu as pltpu
from jax.sharding import Mesh
from jax.sharding import PartitionSpec as P

EPS = 1e-5
N = {"tp": 2, "z": 4, "y": 4, "x": 4}
D = 576
DP = 640
HALF = 512
T = 2 * HALF
VSH = 24576
VB = 128
SVB, DVB, SUB = 2048, 2048, 512
K = 12
NP = 4
YR = 144
RH = 72
LANES = 128
HUGE = 3.0e38
LOG2E, LN2 = 1.4426950408889634, 0.6931471805599453
COLORS = (("yzx", (24, 24)), ("xzy", (24, 24)), ("xyz", (16, 8)), ("yxz", (8, 16)))
BOTH = ((0, 1), (1, 3))
F32, BF16 = jnp.float32, jnp.bfloat16
FAR = (1, 3, 2)
PAIR, TRIPLE = range(2), range(3)
FEW, SOME = 16, 32


def mean0(x):
    return jnp.sum(x, axis=0, keepdims=True) * (1.0 / D)


def fold1(op, x):
    return op(x, axis=1, keepdims=True)


def along(axis, *shape):
    return pl.BlockSpec(shape, lambda s: tuple(s if i == axis else 0 for i in range(len(shape))))


def dot(a, b):
    return lax.dot_general(a, b, (((1,), (0,)), ((), ())), preferred_element_type=F32)


def dot_nt(a, b):
    return lax.dot_general(a, b, (((1,), (1,)), ((), ())), preferred_element_type=F32)


def pos(axis, by=0):
    return lax.rem(lax.axis_index(axis) + by, N[axis])


def peers(axis):
    return FAR[: N[axis] - 1]


def whole(shape, **kw):
    return pl.BlockSpec(shape, lambda *_: (0,) * len(shape), **kw)


ANY = pl.BlockSpec(memory_space=pl.ANY)


def push(src, dst, send, recv, axis, by):
    pltpu.make_async_remote_copy(
        src_ref=src,
        dst_ref=dst,
        send_sem=send,
        recv_sem=recv,
        device_id={axis: pos(axis, by)},
        device_id_type=pl.DeviceIdType.MESH,
    ).start()


def wait(ref, sem):
    pltpu.make_async_copy(ref, ref, sem).wait()


def enter():
    barrier = pltpu.get_barrier_semaphore()
    count = 0
    for axis in N:
        for by in peers(axis):
            pl.semaphore_signal(
                barrier, inc=1, device_id={axis: pos(axis, by)}, device_id_type=pl.DeviceIdType.MESH
            )
            count += 1
    pl.semaphore_wait(barrier, count)


def total(step, axes, own, got, send, recv):
    if step > 0:
        acc = own[step - 1]
        for i, _ in enumerate(peers(axes[step - 1])):
            wait(got.at[step - 1, i], recv.at[step - 1, i])
            wait(got.at[step - 1, i], send.at[step - 1, i])
        for i, _ in enumerate(peers(axes[step - 1])):
            acc = acc + got[step - 1, i]
        own[step] = acc
    if step < len(axes):
        for i, by in enumerate(peers(axes[step])):
            push(own.at[step], got.at[step, i], send.at[step, i], recv.at[step, i], axes[step], by)


def params(**kw):
    return pltpu.CompilerParams(vmem_limit_bytes=63 << 20, **kw)


def cost(flops, nbytes):
    return pl.CostEstimate(flops=int(flops), bytes_accessed=int(nbytes), transcendentals=0)


def norm_kernel(h_ref, g_ref, u_ref, ut_ref, pay_ref):
    h = h_ref[0].astype(F32)
    inv = lax.rsqrt(mean0(h * h) + EPS)
    n = h * inv * g_ref[...]

    @pl.when(pl.program_id(0) == lax.axis_index("tp"))
    def _():
        pay_ref[...] = n

    ut_ref[...] = n.astype(BF16)
    u_ref[...] = n.T.astype(BF16)


def norm_call(hid_t, gain):
    return pl.pallas_call(
        norm_kernel,
        grid=(2,),
        in_specs=[along(0, 1, D, HALF), whole((D, 1))],
        out_specs=[
            along(0, HALF, D),
            along(1, D, HALF),
            whole((D, HALF)),
        ],
        out_shape=[
            jax.ShapeDtypeStruct((T, D), BF16),
            jax.ShapeDtypeStruct((D, T), BF16),
            jax.ShapeDtypeStruct((D, HALF), F32),
        ],
        compiler_params=params(),
        name="norm",
    )(hid_t, gain)


def norm_back_kernel(h_ref, g_ref, du_ref, out_ref):
    h = h_ref[0].astype(F32)
    inv = lax.rsqrt(mean0(h * h) + EPS)
    gdu = (du_ref[0] + du_ref[1]).T[:D] * g_ref[...]
    mean = mean0(h * gdu)
    out_ref[0] = (inv * gdu - h * (inv * inv * inv * mean)).astype(BF16)


def norm_back_call(hid_t, gain, du):
    block = along(0, 1, D, HALF)
    return pl.pallas_call(
        norm_back_kernel,
        grid=(2,),
        in_specs=[block, whole((D, 1)), along(1, 2, HALF, DP)],
        out_specs=block,
        out_shape=jax.ShapeDtypeStruct((2, D, HALF), BF16),
        compiler_params=params(),
        name="norm_back",
    )(hid_t, gain, du)


def stats_kernel(
    pay, mask_ref, lab_ref, u_ref, e_ref, z_ref, rows_ref, out, m_scr, s_scr, own, got, ms, rows_got, ug, *sems
):
    c_send, c_recv, u_send, u_recv, r_send, r_recv, local = sems
    step, steps = pl.program_id(0), pl.num_programs(0)
    cut = D // 2
    near = ((1, 0), (3, 1))

    def at(index, tick):
        pl.when(step == index)(tick)

    def keep(*place):
        pltpu.make_async_copy(ug.at[place], out.at[place], local.at[place]).start()

    def begin():
        m_scr[...] = jnp.full_like(m_scr, -HUGE)
        s_scr[...] = jnp.zeros_like(s_scr)
        own[0] = jnp.broadcast_to(jnp.sum(mask_ref[...].astype(F32)), own.shape[1:])
        enter()
        if N["z"] > 1:
            for by, i in near:
                push(pay, ug.at[0, i], u_send.at[0, i], u_recv.at[0, i], "z", by)
        total(0, "xyz", own, got, c_send, c_recv)

    def pass_on():
        if N["z"] > 1:
            for i in PAIR:
                wait(ug.at[0, i], u_recv.at[0, i])
            for by, i in near:
                piece = pl.ds(i * cut, cut)
                push(ug.at[0, i, piece], ug.at[0, 2, piece], u_send.at[0, 2 + i], u_recv.at[0, 2 + i], "z", by)
                keep(0, i)
                if N["tp"] > 1:
                    push(ug.at[0, i], ug.at[1, i], u_send.at[1, i], u_recv.at[1, i], "tp", 1)

    def share_far():
        if N["z"] > 1:
            for i in PAIR:
                wait(ug.at[0, 2, pl.ds(i * cut, cut)], u_recv.at[0, 2 + i])
            keep(0, 2)
            if N["tp"] > 1:
                push(ug.at[0, 2], ug.at[1, 2], u_send.at[1, 2], u_recv.at[1, 2], "tp", 1)
                for i in PAIR:
                    wait(ug.at[1, i], u_recv.at[1, i])
                    keep(1, i)

    at(0, begin)
    for i in range(1, 4):
        at(i, functools.partial(total, i, "xyz", own, got, c_send, c_recv))
    at(steps * 7 // 12, pass_on)
    at(steps - 1, share_far)

    def fold(k):
        for r in range(0, T, SOME):
            rows = slice(r, r + SOME)
            parts = [z_ref[rows, j : j + LANES] for j in range(k * SUB, (k + 1) * SUB, LANES)]
            old = m_scr[rows, :]
            new = functools.reduce(jnp.maximum, parts, old)
            acc = s_scr[rows, :] * jnp.exp2(old - new)
            for p in parts:
                acc = acc + jnp.exp2(p - new)
            m_scr[rows, :] = new
            s_scr[rows, :] = acc

    for k in range(SVB // SUB):
        z_ref[:, k * SUB : (k + 1) * SUB] = dot(u_ref[...], e_ref[:, k * SUB : (k + 1) * SUB]) * LOG2E
        if k:
            fold(k - 1)
    fold(SVB // SUB - 1)

    @pl.when(step == steps - 1)
    def _():
        m_lane = m_scr[...]
        m_row = fold1(jnp.max, m_lane)
        s_row = fold1(jnp.sum, s_scr[...] * jnp.exp2(m_lane - m_row))
        for i, row in enumerate((m_row, s_row)):
            ms[0, 8 * i : 8 * (i + 1)] = jnp.broadcast_to(row, (T, LANES)).T[:8]
        if N["tp"] > 1:
            push(ms.at[0], ms.at[1], r_send.at[3], r_recv.at[3], "tp", 1)
            wait(ms.at[1], r_recv.at[3])
            wait(ms.at[0], r_send.at[3])
        count = own[3, :1, :1]
        rows_ref[0, 3:8, :] = jnp.broadcast_to(1.0 / count, (5, T))
        swap = lax.axis_index("tp") == 1
        for k in PAIR:
            here = slice(k * HALF, (k + 1) * HALF)
            mask = mask_ref[k : k + 1, :].astype(F32)
            top, whole_sum = ms[0, :1, here], ms[0, 8:9, here]
            if N["tp"] > 1:
                m1, m2 = top, ms[1, :1, here]
                top = jnp.maximum(m1, m2)
                a, b = whole_sum * jnp.exp2(m1 - top), ms[1, 8:9, here] * jnp.exp2(m2 - top)
                whole_sum = jnp.where(swap, b + a, a + b)
            counts = mask > 0.0
            lse = top + jnp.log(whole_sum) * LOG2E
            rows_ref[0, :1, here] = jnp.where(counts, lse + jnp.log(count) * LOG2E, HUGE)
            rows_ref[0, 1:2, here] = jnp.where(counts, lab_ref[k : k + 1, :].astype(F32), -1.0)
            rows_ref[0, 2:3, here] = mask * lse * LN2
        rows_got[0] = rows_ref[0]
        for i, by in enumerate(peers("z")):
            push(rows_got.at[0], rows_got.at[1 + i], r_send.at[i], r_recv.at[i], "z", by)
        for i, _ in enumerate(peers("z")):
            wait(rows_got.at[1 + i], r_recv.at[i])
            wait(rows_got.at[0], r_send.at[i])
            rows_ref[1 + i] = rows_got[1 + i]
        if N["z"] > 1:
            for i in PAIR:
                wait(pay, u_send.at[0, i])
                wait(ug.at[0, 2, pl.ds(i * cut, cut)], u_send.at[0, 2 + i])
            if N["tp"] > 1:
                wait(ug.at[1, 2], u_recv.at[1, 2])
                keep(1, 2)
                for i in TRIPLE:
                    wait(ug.at[0, i], u_send.at[1, i])
                    wait(ug.at[1, i], local.at[1, i])
            for i in TRIPLE:
                wait(ug.at[0, i], local.at[0, i])


def stats_call(pay, mask, lab, u, emb_t):
    dma = pltpu.SemaphoreType.DMA
    return pl.pallas_call(
        stats_kernel,
        grid=(VSH // SVB,),
        in_specs=[
            whole((D, HALF)),
            whole((2, HALF)),
            whole((2, HALF)),
            whole((T, D)),
            along(1, D, SVB),
        ],
        out_specs=[along(1, T, SVB), whole((N["z"], 8, T)), ANY],
        out_shape=[
            jax.ShapeDtypeStruct((T, VSH), F32),
            jax.ShapeDtypeStruct((N["z"], 8, T), F32),
            jax.ShapeDtypeStruct((2, 3, D, HALF), F32),
        ],
        scratch_shapes=[
            pltpu.VMEM((T, LANES), F32),
            pltpu.VMEM((T, LANES), F32),
            pltpu.VMEM((4, 8, LANES), F32),
            pltpu.VMEM((3, 3, 8, LANES), F32),
            pltpu.VMEM((2, 16, T), F32),
            pltpu.VMEM((4, 8, T), F32),
            pltpu.VMEM((2, 3, D, HALF), F32),
            dma((3, 3)),
            dma((3, 3)),
            dma((2, 4)),
            dma((2, 4)),
            dma((4,)),
            dma((4,)),
            dma((2, 3)),
        ],
        compiler_params=params(collective_id=1, has_side_effects=True),
        cost_estimate=cost(2 * T * D * VSH, T * VSH * 4),
        name="stats",
    )(pay, mask, lab, u, emb_t)


def pack_kernel(u_ref, ut_ref, own_ref, sib_ref, u_out, ut_out):
    r = pl.program_id(0)

    @pl.when(r == 0)
    def _():
        u_out[...] = u_ref[...]
        ut_out[...] = ut_ref[...]

    @pl.when(r > 0)
    def _():
        me = lax.axis_index("tp")
        for src, half in ((own_ref, me), (sib_ref, 1 - me)):
            n = src[0, 0]
            here = pl.ds(pl.multiple_of(half * HALF, HALF), HALF)
            ut_out[:, here] = n.astype(BF16)
            u_out[here, :] = n.T.astype(BF16)


def pack_call(u, ut, ug):
    piece = [pl.BlockSpec((1, 1, D, HALF), lambda r, c=c: (c, jnp.maximum(r - 1, 0), 0, 0)) for c in PAIR]
    return pl.pallas_call(
        pack_kernel,
        grid=(N["z"],),
        in_specs=[whole((T, D)), whole((D, T)), *piece],
        out_specs=[along(0, T, D), along(1, D, T)],
        out_shape=[
            jax.ShapeDtypeStruct((N["z"] * T, D), BF16),
            jax.ShapeDtypeStruct((D, N["z"] * T), BF16),
        ],
        compiler_params=params(),
        name="pack",
    )(u, ut, ug, ug)


def spread(row):
    return jnp.broadcast_to(row, (LANES, row.shape[1])).T


def main_kernel(rows_ref, u_ref, ut_ref, eg_ref, ed_ref, z_hbm, g, du, loss_ref, *scr):
    (st, zs, ds, p, ra1, ra2, rb1, rb2, sums, s_scr, zb, acc, dd, found, own, got) = scr[:16]
    rs_send, rs_recv, ag_send, ag_recv, l_send, l_recv, d_send, d_recv, local, z_sem = scr[16:]
    slot = pl.program_id(0)
    nx, ny = N["x"], N["y"]
    dus = VSH // DVB
    wg = nx * VB
    quarter = VSH // N["z"]
    parts = tuple(enumerate(("xy", "yx"))) if nx > 1 else ()
    cut = RH // 16 * 8


    def block(part, k, i, half=None):
        two = slice(None) if half is None else pl.ds(2 * half, 2)
        if part == 0:
            return p.at[lax.rem(k, NP), i, two, pl.ds(0, RH)]
        return p.at[lax.rem(k, NP), two, i, pl.ds(RH, RH)]

    def line(part, k, i, half=None):
        rows = (slice(None), pl.ds(0, cut), pl.ds(cut, RH - cut))[0 if half is None else 1 + half]
        return sums.at[lax.rem(k, NP), part, i, rows]

    def rs_push(k, part, stage, src, dst, axis, by):
        push(src, dst, rs_send.at[k, part], rs_recv.at[k, part, stage], axis, by)

    def rb1_at(k, part, half):
        return rb1.at[k, part, pl.ds(half * cut, RH - cut if half else cut)]

    def reduce_start(k):
        for part, (axis, _) in parts:
            for half, by in BOTH:
                rs_push(k, part, 0, block(part, k, pos(axis, 2), half), ra1.at[k, part, half], axis, by)

    def reduce_pass(k):
        for part, (axis, _) in parts:
            wait(ra1.at[k, part], rs_recv.at[k, part, 0])
            for half, by in BOTH:
                block(part, k, pos(axis, by), half)[...] += ra1[k, part, half]
        for part, (axis, _) in parts:
            for half, by in BOTH:
                rs_push(k, part, 1, block(part, k, pos(axis, by)), ra2.at[k, part, half], axis, by)

    def reduce_turn(k):
        for part, (axis, _) in parts:
            wait(ra2.at[k, part], rs_recv.at[k, part, 1])
            sums[lax.rem(k, NP), part] = block(part, k, pos(axis))[...] + ra2[k, part, 0] + ra2[k, part, 1]
        for part, (_, axis) in parts:
            for half, by in BOTH:
                rs_push(k, part, 2, line(part, k, pos(axis, 2), half), rb1_at(k, part, half), axis, by)

    def reduce_pass2(k):
        for part, (_, axis) in parts:
            wait(rb1.at[k, part], rs_recv.at[k, part, 2])
            for half, by in BOTH:
                line(part, k, pos(axis, by), half)[...] += rb1_at(k, part, half)[...]
        for part, (_, axis) in parts:
            for half, by in BOTH:
                rs_push(k, part, 3, line(part, k, pos(axis, by)), rb2.at[k, part, half], axis, by)

    def reduce_end(k):
        if not parts:
            s_scr[k] = p[lax.rem(k, NP), 0, 0]
        for part, (_, axis) in parts:
            wait(rb2.at[k, part], rs_recv.at[k, part, 3])
            s_scr[k, pl.ds(part * RH, RH)] = line(part, k, pos(axis))[...] + rb2[k, part, 0] + rb2[k, part, 1]
            wait(g.at[0, pl.ds(0, RH), pl.ds(0, 15 * VB)], rs_send.at[k, part])
        here = pl.ds(pl.multiple_of(pos("z") * quarter + k * wg + pos("x") * VB, LANES), VB)
        pltpu.make_async_copy(s_scr.at[k], g.at[pos("y"), :, here], local).start()
        wait(s_scr.at[k], local)


    def areas(k, color, phase, v, half=None):
        order, rows = COLORS[color]
        place = {a: pos(a) for a in "xyz"}
        for a in order[:phase]:
            place[a] = None
        place[order[phase]] = v
        row0, n = sum(sum(c[1]) for c in COLORS[:color]), sum(rows)
        if half is not None:
            row0, n = row0 + half * rows[0], rows[half]
        ys = slice(None) if place["y"] is None else pl.ds(place["y"], 1)
        for z in range(N["z"]) if place["z"] is None else (place["z"],):
            col, width = z * quarter + k * wg, wg
            if place["x"] is not None:
                col, width = col + place["x"] * VB, VB
            yield g.at[ys, pl.ds(row0, n), pl.ds(pl.multiple_of(col, LANES), width)]

    def units(color, phase):
        n = 1
        for a in COLORS[color][0][:phase]:
            n *= N[a]
        return n

    def bulk(color, count, part=None):
        rows = COLORS[color][1]
        n = sum(rows) if part is None else rows[part]
        return g.at[0, pl.ds(0, n), pl.ds(0, count * VB)]

    def near(k, c, phase):
        axis = COLORS[c][0][phase]
        if phase > 0:
            far_done(k, c, phase - 1)
        if N[axis] > 1:
            for _, by in BOTH:
                for src in areas(k, c, phase, pos(axis)):
                    push(src, src, ag_send.at[k, c], ag_recv.at[k, c, 2 * phase], axis, by)

    def far(k, c, phase):
        axis = COLORS[c][0][phase]
        if N[axis] > 1:
            wait(bulk(c, 2 * units(c, phase)), ag_recv.at[k, c, 2 * phase])
            for half, by in BOTH:
                for src in areas(k, c, phase, pos(axis, N[axis] - by), half):
                    push(src, src, ag_send.at[k, c], ag_recv.at[k, c, 2 * phase + 1], axis, by)

    def far_done(k, c, phase):
        if N[COLORS[c][0][phase]] > 1:
            wait(bulk(c, units(c, phase)), ag_recv.at[k, c, 2 * phase + 1])

    def gather_end(k, c):
        far_done(k, c, 2)
        count = sum(3 * units(c, i) for i in TRIPLE if N[COLORS[c][0][i]] > 1)
        wait(bulk(c, count), ag_send.at[k, c])

    reduces = (reduce_start, reduce_pass, reduce_turn, reduce_pass2, reduce_end)

    def stage(index, tick, *args):
        since = slot - 1 - index

        @pl.when((since >= 0) & (lax.rem(since, 2) == 0) & (since < 2 * K))
        def _():
            tick(since // 2, *args)

    def fetch(i):
        pltpu.make_async_copy(z_hbm.at[:, pl.ds(pl.multiple_of(i * DVB, LANES), DVB)], zb, z_sem).start()

    @pl.when(slot == 0)
    def _():
        fetch(0)
        for r in range(N["z"]):
            for k in PAIR:
                st[k, r * T : (r + 1) * T, :] = spread(rows_ref[r, k : k + 1, :])
        acc[...] = jnp.zeros_like(acc)
        found[...] = jnp.zeros_like(found)
        enter()

    for c in range(len(COLORS)):
        for phase in TRIPLE:
            stage(len(reduces) + 2 * phase, near, c, phase)
            stage(len(reduces) + 2 * phase + 1, far, c, phase)
        stage(len(reduces) + 6, gather_end, c)
    for i, tick in enumerate(reduces):
        stage(i, tick)

    hit_value = rows_ref[0, 3:4, :LANES]

    @pl.when((slot < 2 * K) & (lax.rem(slot, 2) == 0))
    def _():
        k = slot // 2
        buf = lax.rem(k, NP)
        base = lax.axis_index("tp") * VSH + lax.axis_index("z") * quarter + k * wg
        ids = (lax.broadcasted_iota(jnp.int32, (FEW, wg), 1) + base).astype(F32)
        hit_row = jnp.concatenate([hit_value] * nx, axis=1)

        def logits(h, t0):
            zs[h] = dot(u_ref[pl.ds(t0, HALF), :], eg_ref[...])

        def deltas(h, t0):
            for r in range(0, HALF, FEW):
                here = pl.ds(t0 + r, FEW)
                lse, label = (jnp.concatenate([st[i, here, :]] * nx, axis=1) for i in PAIR)
                e = jnp.exp2(zs[h, r : r + FEW, :] * LOG2E - lse)
                ds[h, r : r + FEW, :] = jnp.where(label == ids, e - hit_row, e).astype(BF16)

        def product(h, t0):
            part = dot(ut_ref[:, pl.ds(t0, HALF)], ds[h]).reshape(ny, YR, wg)
            for i in range(nx):
                p[buf, i] += part[:, :, i * VB : (i + 1) * VB]

        p[buf] = jnp.zeros(p.shape[1:], F32)

        @pl.loop(0, N["z"])
        def _(r):
            ta = pl.multiple_of(r * T, T)
            tb = pl.multiple_of(r * T + HALF, HALF)
            logits(0, ta)
            logits(1, tb)
            deltas(0, ta)
            product(0, ta)
            deltas(1, tb)
            product(1, tb)

    @pl.when((slot < 2 * dus) & (lax.rem(slot, 2) == 1))
    def _():
        i = slot // 2
        wait(zb, z_sem)
        base = lax.axis_index("tp") * VSH + i * DVB
        ids0 = lax.broadcasted_iota(jnp.int32, (SOME, LANES), 1) + base
        for k in range(DVB // SUB):
            cols = slice(k * SUB, (k + 1) * SUB)
            ids = [(ids0 + j).astype(F32) for j in range(k * SUB, (k + 1) * SUB, LANES)]
            for r in range(0, T, SOME):
                here = slice(r, r + SOME)
                lse, label = (st[n, here, :] for n in PAIR)
                hits = found[here, :]
                for j, idj in enumerate(ids):
                    z = zb[here, k * SUB + j * LANES : k * SUB + (j + 1) * LANES]
                    e = jnp.exp2(z - lse)
                    hit = label == idj
                    hits = jnp.where(hit, z, hits)
                    dd[k % 2, here, j * LANES : (j + 1) * LANES] = jnp.where(hit, e - hit_value, e).astype(BF16)
                found[here, :] = hits
            acc[:, :D] += dot_nt(dd[k % 2], ed_ref[:, cols])

        @pl.when(i + 1 < dus)
        def _():
            fetch(i + 1)


    def finish_du():
        if N["tp"] > 1:
            push(acc, du.at[1], d_send.at[0], d_recv, "tp", 1)
        pltpu.make_async_copy(acc, du.at[0], d_send.at[1]).start()
        logs = jnp.where(lax.axis_index("tp") == 0, jnp.sum(rows_ref[0, 2:3, :]), 0.0)
        own[0] = jnp.broadcast_to(logs - jnp.sum(found[...]) * LN2, own.shape[1:])

    def finish():
        wait(acc, d_send.at[1])
        if N["tp"] > 1:
            wait(acc, d_send.at[0])
            wait(acc, d_recv)
        loss_ref[...] = own[len(AXES)] * hit_value

    pl.when(slot == 2 * dus)(finish_du)
    for i in range(len(AXES) + 1):
        pl.when(slot == 2 * dus + 1 + i)(functools.partial(total, i, AXES, own, got, l_send, l_recv))
    pl.when(slot == pl.num_programs(0) - 1)(finish)


AXES = ("tp", "x", "y", "z")


def main_call(rows, u_all, ut_all, emb_t, logits):
    nx, ny, nz = N["x"], N["y"], N["z"]
    wg = nx * VB
    dus = VSH // DVB
    dma = pltpu.SemaphoreType.DMA

    def grad_block(s):
        return 0, lax.axis_index("z") * K + jnp.minimum(s // 2, K - 1)

    def du_block(s):
        return 0, jnp.minimum(s // 2, dus - 1)

    once = dict(pipeline_mode=pl.Buffered(1))
    return pl.pallas_call(
        main_kernel,
        grid=(2 * K + 12,),
        in_specs=[
            whole((nz, 8, T), **once),
            whole((nz * T, D), **once),
            whole((D, nz * T), **once),
            pl.BlockSpec((D, wg), grad_block),
            pl.BlockSpec((D, DVB), du_block),
            ANY,
        ],
        out_specs=[ANY, ANY, whole((8, LANES))],
        out_shape=[
            jax.ShapeDtypeStruct((ny, YR, VSH), F32),
            jax.ShapeDtypeStruct((2, T, DP), F32),
            jax.ShapeDtypeStruct((8, LANES), F32),
        ],
        scratch_shapes=[
            pltpu.VMEM(shape, F32)
            for shape in (
                (2, nz * T, LANES),
                (2, HALF, wg),
            )
        ]
        + [pltpu.VMEM((2, HALF, wg), BF16)]
        + [
            pltpu.VMEM(shape, F32)
            for shape in (
                (NP, nx, ny, YR, VB),
                (K, 2, 2, 2, RH, VB),
                (K, 2, 2, 4, RH, VB),
                (K, 2, RH, VB),
                (K, 2, 2, RH, VB),
                (NP, 2, 4, RH, VB),
                (K, YR, VB),
                (T, DVB),
                (T, DP),
            )
        ]
        + [
            pltpu.VMEM((2, T, SUB), BF16),
            pltpu.VMEM((T, LANES), F32),
            pltpu.VMEM((5, 8, LANES), F32),
            pltpu.VMEM((4, 3, 8, LANES), F32),
            dma((K, 2)),
            dma((K, 2, 4)),
            dma((K, len(COLORS))),
            dma((K, len(COLORS), 6)),
            dma((4, 3)),
            dma((4, 3)),
            dma((2,)),
            dma,
            dma,
            dma,
        ],
        compiler_params=params(collective_id=2, has_side_effects=True),
        cost_estimate=cost(6 * T * D * VSH, T * VSH * 4),
        name="main",
    )(rows, u_all, ut_all, emb_t, emb_t, logits)


def solution(mesh):
    axes = tuple(N)
    grid_mesh = Mesh(mesh.devices.reshape(tuple(N.values())), axes)

    def local_body(hidden, labels, loss_mask, norm_gain, embedding):
        emb_t = embedding.T
        hid_t = hidden.transpose(0, 2, 1)
        gain = norm_gain.astype(F32)[:, None]
        u, ut, pay = norm_call(hid_t, gain)
        logits, rows, ug = stats_call(pay, loss_mask, labels, u, emb_t)
        u_all, ut_all = pack_call(u, ut, ug)
        grad, du, loss = main_call(rows, u_all, ut_all, emb_t, logits)
        d_hidden = norm_back_call(hid_t, gain, du)
        return loss[0, 0], d_hidden.transpose(0, 2, 1), grad.reshape(D, VSH).T

    dp = axes[1:]
    return jax.shard_map(
        local_body,
        mesh=grid_mesh,
        in_specs=(P(dp), P(dp), P(dp), P(), P("tp")),
        out_specs=(P(), P(dp), P("tp")),
        check_vma=False,
    )
```

```python
import functools

import jax
import jax.numpy as jnp
from jax import lax
from jax.experimental import pallas as pl
from jax.experimental.pallas import tpu as pltpu
from jax.sharding import Mesh
from jax.sharding import PartitionSpec as P

EPS = 1e-5
N = {"tp": 2, "z": 4, "y": 4, "x": 4}
D = 576
DP = 640
HALF = 512
T = 2 * HALF
VSH = 24576
VB = 128
SVB, DVB, SUB = 2048, 2048, 512
K = 12
NP = 4
YR = 144
RH = 72
LANES = 128
HUGE = 3.0e38
COLORS = (("yzx", (24, 24)), ("xzy", (24, 24)), ("xyz", (16, 8)), ("yxz", (8, 16)))
BOTH = ((0, 1), (1, 3))
F32, BF16 = jnp.float32, jnp.bfloat16
FAR = (1, 3, 2)
PAIR, TRIPLE = range(2), range(3)
FEW, SOME = 16, 32


def mean0(x):
    return jnp.sum(x, axis=0, keepdims=True) * (1.0 / D)


def fold1(op, x):
    return op(x, axis=1, keepdims=True)


def along(axis, *shape):
    return pl.BlockSpec(shape, lambda s: tuple(s if i == axis else 0 for i in range(len(shape))))


def dot(a, b):
    return lax.dot_general(a, b, (((1,), (0,)), ((), ())), preferred_element_type=F32)


def dot_nt(a, b):
    return lax.dot_general(a, b, (((1,), (1,)), ((), ())), preferred_element_type=F32)


def pos(axis, by=0):
    return lax.rem(lax.axis_index(axis) + by, N[axis])


def peers(axis):
    return FAR[: N[axis] - 1]


def whole(shape, **kw):
    return pl.BlockSpec(shape, lambda *_: (0,) * len(shape), **kw)


ANY = pl.BlockSpec(memory_space=pl.ANY)


def push(src, dst, send, recv, axis, by):
    pltpu.make_async_remote_copy(
        src_ref=src,
        dst_ref=dst,
        send_sem=send,
        recv_sem=recv,
        device_id={axis: pos(axis, by)},
        device_id_type=pl.DeviceIdType.MESH,
    ).start()


def wait(ref, sem):
    pltpu.make_async_copy(ref, ref, sem).wait()


def enter():
    barrier = pltpu.get_barrier_semaphore()
    count = 0
    for axis in N:
        for by in peers(axis):
            pl.semaphore_signal(
                barrier, inc=1, device_id={axis: pos(axis, by)}, device_id_type=pl.DeviceIdType.MESH
            )
            count += 1
    pl.semaphore_wait(barrier, count)


def total(step, axes, own, got, send, recv):
    if step > 0:
        acc = own[step - 1]
        for i, _ in enumerate(peers(axes[step - 1])):
            wait(got.at[step - 1, i], recv.at[step - 1, i])
            wait(got.at[step - 1, i], send.at[step - 1, i])
        for i, _ in enumerate(peers(axes[step - 1])):
            acc = acc + got[step - 1, i]
        own[step] = acc
    if step < len(axes):
        for i, by in enumerate(peers(axes[step])):
            push(own.at[step], got.at[step, i], send.at[step, i], recv.at[step, i], axes[step], by)


def params(**kw):
    return pltpu.CompilerParams(vmem_limit_bytes=63 << 20, **kw)


def cost(flops, nbytes):
    return pl.CostEstimate(flops=int(flops), bytes_accessed=int(nbytes), transcendentals=0)


def norm_kernel(h_ref, g_ref, u_ref, ut_ref, pay_ref):
    h = h_ref[0].astype(F32)
    inv = lax.rsqrt(mean0(h * h) + EPS)
    n = h * inv * g_ref[...]

    @pl.when(pl.program_id(0) == lax.axis_index("tp"))
    def _():
        pay_ref[...] = n

    ut_ref[...] = n.astype(BF16)
    u_ref[...] = n.T.astype(BF16)


def norm_call(hid_t, gain):
    return pl.pallas_call(
        norm_kernel,
        grid=(2,),
        in_specs=[along(0, 1, D, HALF), whole((D, 1))],
        out_specs=[
            along(0, HALF, D),
            along(1, D, HALF),
            whole((D, HALF)),
        ],
        out_shape=[
            jax.ShapeDtypeStruct((T, D), BF16),
            jax.ShapeDtypeStruct((D, T), BF16),
            jax.ShapeDtypeStruct((D, HALF), F32),
        ],
        compiler_params=params(),
        name="norm",
    )(hid_t, gain)


def norm_back_kernel(h_ref, g_ref, du_ref, out_ref):
    h = h_ref[0].astype(F32)
    inv = lax.rsqrt(mean0(h * h) + EPS)
    gdu = (du_ref[0] + du_ref[1]).T[:D] * g_ref[...]
    mean = mean0(h * gdu)
    out_ref[0] = (inv * gdu - h * (inv * inv * inv * mean)).astype(BF16)


def norm_back_call(hid_t, gain, du):
    block = along(0, 1, D, HALF)
    return pl.pallas_call(
        norm_back_kernel,
        grid=(2,),
        in_specs=[block, whole((D, 1)), along(1, 2, HALF, DP)],
        out_specs=block,
        out_shape=jax.ShapeDtypeStruct((2, D, HALF), BF16),
        compiler_params=params(),
        name="norm_back",
    )(hid_t, gain, du)


def stats_kernel(
    pay, mask_ref, lab_ref, u_ref, e_ref, z_ref, rows_ref, out, m_scr, s_scr, own, got, ms, rows_got, ug, *sems
):
    c_send, c_recv, u_send, u_recv, r_send, r_recv, local = sems
    step, steps = pl.program_id(0), pl.num_programs(0)
    cut = D // 2
    near = ((1, 0), (3, 1))

    def at(index, tick):
        pl.when(step == index)(tick)

    def keep(*place):
        pltpu.make_async_copy(ug.at[place], out.at[place], local.at[place]).start()

    def begin():
        m_scr[...] = jnp.full_like(m_scr, -HUGE)
        s_scr[...] = jnp.zeros_like(s_scr)
        own[0] = jnp.broadcast_to(jnp.sum(mask_ref[...].astype(F32)), own.shape[1:])
        enter()
        if N["z"] > 1:
            for by, i in near:
                push(pay, ug.at[0, i], u_send.at[0, i], u_recv.at[0, i], "z", by)
        total(0, "xyz", own, got, c_send, c_recv)

    def pass_on():
        if N["z"] > 1:
            for i in PAIR:
                wait(ug.at[0, i], u_recv.at[0, i])
            for by, i in near:
                piece = pl.ds(i * cut, cut)
                push(ug.at[0, i, piece], ug.at[0, 2, piece], u_send.at[0, 2 + i], u_recv.at[0, 2 + i], "z", by)
                keep(0, i)
                if N["tp"] > 1:
                    push(ug.at[0, i], ug.at[1, i], u_send.at[1, i], u_recv.at[1, i], "tp", 1)

    def share_far():
        if N["z"] > 1:
            for i in PAIR:
                wait(ug.at[0, 2, pl.ds(i * cut, cut)], u_recv.at[0, 2 + i])
            keep(0, 2)
            if N["tp"] > 1:
                push(ug.at[0, 2], ug.at[1, 2], u_send.at[1, 2], u_recv.at[1, 2], "tp", 1)
                for i in PAIR:
                    wait(ug.at[1, i], u_recv.at[1, i])
                    keep(1, i)

    at(0, begin)
    for i, when in enumerate((1, 2, steps - 2)):
        at(when, functools.partial(total, i + 1, "xyz", own, got, c_send, c_recv))
    at(steps * 7 // 12, pass_on)
    at(steps - 1, share_far)

    def fold(k):
        for r in range(0, T, SOME):
            rows = slice(r, r + SOME)
            parts = [z_ref[rows, j : j + LANES] for j in range(k * SUB, (k + 1) * SUB, LANES)]
            old = m_scr[rows, :]
            new = functools.reduce(jnp.maximum, parts, old)
            acc = s_scr[rows, :] * jnp.exp(old - new)
            for p in parts:
                acc = acc + jnp.exp(p - new)
            m_scr[rows, :] = new
            s_scr[rows, :] = acc

    for k in range(SVB // SUB):
        z_ref[:, k * SUB : (k + 1) * SUB] = dot(u_ref[...], e_ref[:, k * SUB : (k + 1) * SUB])
        if k:
            fold(k - 1)
    fold(SVB // SUB - 1)

    @pl.when(step == steps - 1)
    def _():
        m_lane = m_scr[...]
        m_row = fold1(jnp.max, m_lane)
        s_row = fold1(jnp.sum, s_scr[...] * jnp.exp(m_lane - m_row))
        for i, row in enumerate((m_row, s_row)):
            ms[0, 8 * i : 8 * (i + 1)] = jnp.broadcast_to(row, (T, LANES)).T[:8]
        if N["tp"] > 1:
            push(ms.at[0], ms.at[1], r_send.at[3], r_recv.at[3], "tp", 1)
            wait(ms.at[1], r_recv.at[3])
            wait(ms.at[0], r_send.at[3])
        count = own[3, :1, :1]
        rows_ref[0, 3:8, :] = jnp.broadcast_to(1.0 / count, (5, T))
        swap = lax.axis_index("tp") == 1
        for k in PAIR:
            here = slice(k * HALF, (k + 1) * HALF)
            mask = mask_ref[k : k + 1, :].astype(F32)
            top, whole_sum = ms[0, :1, here], ms[0, 8:9, here]
            if N["tp"] > 1:
                m1, m2 = top, ms[1, :1, here]
                top = jnp.maximum(m1, m2)
                a, b = whole_sum * jnp.exp(m1 - top), ms[1, 8:9, here] * jnp.exp(m2 - top)
                whole_sum = jnp.where(swap, b + a, a + b)
            counts = mask > 0.0
            lse = top + jnp.log(whole_sum)
            rows_ref[0, :1, here] = jnp.where(counts, lse + jnp.log(count), HUGE)
            rows_ref[0, 1:2, here] = jnp.where(counts, lab_ref[k : k + 1, :].astype(F32), -1.0)
            rows_ref[0, 2:3, here] = mask * lse
        rows_got[0] = rows_ref[0]
        for i, by in enumerate(peers("z")):
            push(rows_got.at[0], rows_got.at[1 + i], r_send.at[i], r_recv.at[i], "z", by)
        for i, _ in enumerate(peers("z")):
            wait(rows_got.at[1 + i], r_recv.at[i])
            wait(rows_got.at[0], r_send.at[i])
            rows_ref[1 + i] = rows_got[1 + i]
        if N["z"] > 1:
            for i in PAIR:
                wait(pay, u_send.at[0, i])
                wait(ug.at[0, 2, pl.ds(i * cut, cut)], u_send.at[0, 2 + i])
            if N["tp"] > 1:
                wait(ug.at[1, 2], u_recv.at[1, 2])
                keep(1, 2)
                for i in TRIPLE:
                    wait(ug.at[0, i], u_send.at[1, i])
                    wait(ug.at[1, i], local.at[1, i])
            for i in TRIPLE:
                wait(ug.at[0, i], local.at[0, i])


def stats_call(pay, mask, lab, u, emb_t):
    dma = pltpu.SemaphoreType.DMA
    return pl.pallas_call(
        stats_kernel,
        grid=(VSH // SVB,),
        in_specs=[
            whole((D, HALF)),
            whole((2, HALF)),
            whole((2, HALF)),
            whole((T, D)),
            along(1, D, SVB),
        ],
        out_specs=[along(1, T, SVB), whole((N["z"], 8, T)), ANY],
        out_shape=[
            jax.ShapeDtypeStruct((T, VSH), F32),
            jax.ShapeDtypeStruct((N["z"], 8, T), F32),
            jax.ShapeDtypeStruct((2, 3, D, HALF), F32),
        ],
        scratch_shapes=[
            pltpu.VMEM((T, LANES), F32),
            pltpu.VMEM((T, LANES), F32),
            pltpu.VMEM((4, 8, LANES), F32),
            pltpu.VMEM((3, 3, 8, LANES), F32),
            pltpu.VMEM((2, 16, T), F32),
            pltpu.VMEM((4, 8, T), F32),
            pltpu.VMEM((2, 3, D, HALF), F32),
            dma((3, 3)),
            dma((3, 3)),
            dma((2, 4)),
            dma((2, 4)),
            dma((4,)),
            dma((4,)),
            dma((2, 3)),
        ],
        compiler_params=params(collective_id=1, has_side_effects=True),
        cost_estimate=cost(2 * T * D * VSH, T * VSH * 4),
        name="stats",
    )(pay, mask, lab, u, emb_t)


def pack_kernel(u_ref, ut_ref, own_ref, sib_ref, u_out, ut_out):
    r = pl.program_id(0)

    @pl.when(r == 0)
    def _():
        u_out[...] = u_ref[...]
        ut_out[...] = ut_ref[...]

    @pl.when(r > 0)
    def _():
        me = lax.axis_index("tp")
        for src, half in ((own_ref, me), (sib_ref, 1 - me)):
            n = src[0, 0]
            here = pl.ds(pl.multiple_of(half * HALF, HALF), HALF)
            ut_out[:, here] = n.astype(BF16)
            u_out[here, :] = n.T.astype(BF16)


def pack_call(u, ut, ug):
    piece = [pl.BlockSpec((1, 1, D, HALF), lambda r, c=c: (c, jnp.maximum(r - 1, 0), 0, 0)) for c in PAIR]
    return pl.pallas_call(
        pack_kernel,
        grid=(N["z"],),
        in_specs=[whole((T, D)), whole((D, T)), *piece],
        out_specs=[along(0, T, D), along(1, D, T)],
        out_shape=[
            jax.ShapeDtypeStruct((N["z"] * T, D), BF16),
            jax.ShapeDtypeStruct((D, N["z"] * T), BF16),
        ],
        compiler_params=params(),
        name="pack",
    )(u, ut, ug, ug)


def spread(row):
    return jnp.broadcast_to(row, (LANES, row.shape[1])).T


def main_kernel(rows_ref, u_ref, ut_ref, eg_ref, ed_ref, z_hbm, g, du, loss_ref, *scr):
    (st, zs, ds, p, ra1, ra2, rb1, rb2, sums, s_scr, zb, acc, dd, found, own, got) = scr[:16]
    rs_send, rs_recv, ag_send, ag_recv, l_send, l_recv, d_send, d_recv, local, z_sem = scr[16:]
    slot = pl.program_id(0)
    nx, ny = N["x"], N["y"]
    dus = VSH // DVB
    wg = nx * VB
    quarter = VSH // N["z"]
    parts = tuple(enumerate(("xy", "yx"))) if nx > 1 else ()
    cut = RH // 16 * 8


    def block(part, k, i, half=None):
        two = slice(None) if half is None else pl.ds(2 * half, 2)
        if part == 0:
            return p.at[lax.rem(k, NP), i, two, pl.ds(0, RH)]
        return p.at[lax.rem(k, NP), two, i, pl.ds(RH, RH)]

    def line(part, k, i, half=None):
        rows = (slice(None), pl.ds(0, cut), pl.ds(cut, RH - cut))[0 if half is None else 1 + half]
        return sums.at[lax.rem(k, NP), part, i, rows]

    def rs_push(k, part, stage, src, dst, axis, by):
        push(src, dst, rs_send.at[k, part], rs_recv.at[k, part, stage], axis, by)

    def rb1_at(k, part, half):
        return rb1.at[k, part, pl.ds(half * cut, RH - cut if half else cut)]

    def reduce_start(k):
        for part, (axis, _) in parts:
            for half, by in BOTH:
                rs_push(k, part, 0, block(part, k, pos(axis, 2), half), ra1.at[k, part, half], axis, by)

    def reduce_pass(k):
        for part, (axis, _) in parts:
            wait(ra1.at[k, part], rs_recv.at[k, part, 0])
            for half, by in BOTH:
                block(part, k, pos(axis, by), half)[...] += ra1[k, part, half]
        for part, (axis, _) in parts:
            for half, by in BOTH:
                rs_push(k, part, 1, block(part, k, pos(axis, by)), ra2.at[k, part, half], axis, by)

    def reduce_turn(k):
        for part, (axis, _) in parts:
            wait(ra2.at[k, part], rs_recv.at[k, part, 1])
            sums[lax.rem(k, NP), part] = block(part, k, pos(axis))[...] + ra2[k, part, 0] + ra2[k, part, 1]
        for part, (_, axis) in parts:
            for half, by in BOTH:
                rs_push(k, part, 2, line(part, k, pos(axis, 2), half), rb1_at(k, part, half), axis, by)

    def reduce_pass2(k):
        for part, (_, axis) in parts:
            wait(rb1.at[k, part], rs_recv.at[k, part, 2])
            for half, by in BOTH:
                line(part, k, pos(axis, by), half)[...] += rb1_at(k, part, half)[...]
        for part, (_, axis) in parts:
            for half, by in BOTH:
                rs_push(k, part, 3, line(part, k, pos(axis, by)), rb2.at[k, part, half], axis, by)

    def reduce_end(k):
        if not parts:
            s_scr[k] = p[lax.rem(k, NP), 0, 0]
        for part, (_, axis) in parts:
            wait(rb2.at[k, part], rs_recv.at[k, part, 3])
            s_scr[k, pl.ds(part * RH, RH)] = line(part, k, pos(axis))[...] + rb2[k, part, 0] + rb2[k, part, 1]
            wait(g.at[0, pl.ds(0, RH), pl.ds(0, 15 * VB)], rs_send.at[k, part])
        here = pl.ds(pl.multiple_of(pos("z") * quarter + k * wg + pos("x") * VB, LANES), VB)
        pltpu.make_async_copy(s_scr.at[k], g.at[pos("y"), :, here], local).start()
        wait(s_scr.at[k], local)


    def areas(k, color, phase, v, half=None):
        order, rows = COLORS[color]
        place = {a: pos(a) for a in "xyz"}
        for a in order[:phase]:
            place[a] = None
        place[order[phase]] = v
        row0, n = sum(sum(c[1]) for c in COLORS[:color]), sum(rows)
        if half is not None:
            row0, n = row0 + half * rows[0], rows[half]
        ys = slice(None) if place["y"] is None else pl.ds(place["y"], 1)
        for z in range(N["z"]) if place["z"] is None else (place["z"],):
            col, width = z * quarter + k * wg, wg
            if place["x"] is not None:
                col, width = col + place["x"] * VB, VB
            yield g.at[ys, pl.ds(row0, n), pl.ds(pl.multiple_of(col, LANES), width)]

    def units(color, phase):
        n = 1
        for a in COLORS[color][0][:phase]:
            n *= N[a]
        return n

    def bulk(color, count, part=None):
        rows = COLORS[color][1]
        n = sum(rows) if part is None else rows[part]
        return g.at[0, pl.ds(0, n), pl.ds(0, count * VB)]

    def near(k, c, phase):
        axis = COLORS[c][0][phase]
        if phase > 0:
            far_done(k, c, phase - 1)
        if N[axis] > 1:
            for _, by in BOTH:
                for src in areas(k, c, phase, pos(axis)):
                    push(src, src, ag_send.at[k, c], ag_recv.at[k, c, 2 * phase], axis, by)

    def far(k, c, phase):
        axis = COLORS[c][0][phase]
        if N[axis] > 1:
            wait(bulk(c, 2 * units(c, phase)), ag_recv.at[k, c, 2 * phase])
            for half, by in BOTH:
                for src in areas(k, c, phase, pos(axis, N[axis] - by), half):
                    push(src, src, ag_send.at[k, c], ag_recv.at[k, c, 2 * phase + 1], axis, by)

    def far_done(k, c, phase):
        if N[COLORS[c][0][phase]] > 1:
            wait(bulk(c, units(c, phase)), ag_recv.at[k, c, 2 * phase + 1])

    def gather_end(k, c):
        far_done(k, c, 2)
        count = sum(3 * units(c, i) for i in TRIPLE if N[COLORS[c][0][i]] > 1)
        wait(bulk(c, count), ag_send.at[k, c])

    reduces = (reduce_start, reduce_pass, reduce_turn, reduce_pass2, reduce_end)

    def stage(index, tick, *args):
        since = slot - 1 - index

        @pl.when((since >= 0) & (lax.rem(since, 2) == 0) & (since < 2 * K))
        def _():
            tick(since // 2, *args)

    def fetch(i):
        pltpu.make_async_copy(z_hbm.at[:, pl.ds(pl.multiple_of(i * DVB, LANES), DVB)], zb, z_sem).start()

    @pl.when(slot == 0)
    def _():
        fetch(0)
        for r in range(N["z"]):
            for k in PAIR:
                st[k, r * T : (r + 1) * T, :] = spread(rows_ref[r, k : k + 1, :])
        acc[...] = jnp.zeros_like(acc)
        found[...] = jnp.zeros_like(found)
        enter()

    for c in range(len(COLORS)):
        for phase in TRIPLE:
            stage(len(reduces) + 2 * phase, near, c, phase)
            stage(len(reduces) + 2 * phase + 1, far, c, phase)
        stage(len(reduces) + 6, gather_end, c)
    for i, tick in enumerate(reduces):
        stage(i, tick)

    hit_value = rows_ref[0, 3:4, :LANES]

    @pl.when((slot < 2 * K) & (lax.rem(slot, 2) == 0))
    def _():
        k = slot // 2
        buf = lax.rem(k, NP)
        base = lax.axis_index("tp") * VSH + lax.axis_index("z") * quarter + k * wg
        ids = (lax.broadcasted_iota(jnp.int32, (FEW, wg), 1) + base).astype(F32)
        hit_row = jnp.concatenate([hit_value] * nx, axis=1)

        def logits(h, t0):
            zs[h] = dot(u_ref[pl.ds(t0, HALF), :], eg_ref[...])

        def deltas(h, t0):
            for r in range(0, HALF, FEW):
                here = pl.ds(t0 + r, FEW)
                lse, label = (jnp.concatenate([st[i, here, :]] * nx, axis=1) for i in PAIR)
                e = jnp.exp(zs[h, r : r + FEW, :] - lse)
                ds[h, r : r + FEW, :] = jnp.where(label == ids, e - hit_row, e).astype(BF16)

        def product(h, t0):
            part = dot(ut_ref[:, pl.ds(t0, HALF)], ds[h]).reshape(ny, YR, wg)
            for i in range(nx):
                p[buf, i] += part[:, :, i * VB : (i + 1) * VB]

        p[buf] = jnp.zeros(p.shape[1:], F32)

        @pl.loop(0, N["z"])
        def _(r):
            ta = pl.multiple_of(r * T, T)
            tb = pl.multiple_of(r * T + HALF, HALF)
            logits(0, ta)
            logits(1, tb)
            deltas(0, ta)
            product(0, ta)
            deltas(1, tb)
            product(1, tb)

    @pl.when((slot < 2 * dus) & (lax.rem(slot, 2) == 1))
    def _():
        i = slot // 2
        wait(zb, z_sem)
        base = lax.axis_index("tp") * VSH + i * DVB
        ids0 = lax.broadcasted_iota(jnp.int32, (SOME, LANES), 1) + base
        for k in range(DVB // SUB):
            cols = slice(k * SUB, (k + 1) * SUB)
            ids = [(ids0 + j).astype(F32) for j in range(k * SUB, (k + 1) * SUB, LANES)]
            for r in range(0, T, SOME):
                here = slice(r, r + SOME)
                lse, label = (st[n, here, :] for n in PAIR)
                hits = found[here, :]
                for j, idj in enumerate(ids):
                    z = zb[here, k * SUB + j * LANES : k * SUB + (j + 1) * LANES]
                    e = jnp.exp(z - lse)
                    hit = label == idj
                    hits = jnp.where(hit, z, hits)
                    dd[k % 2, here, j * LANES : (j + 1) * LANES] = jnp.where(hit, e - hit_value, e).astype(BF16)
                found[here, :] = hits
            acc[:, :D] += dot_nt(dd[k % 2], ed_ref[:, cols])

        @pl.when(i + 1 < dus)
        def _():
            fetch(i + 1)


    def finish_du():
        if N["tp"] > 1:
            push(acc, du.at[1], d_send.at[0], d_recv, "tp", 1)
        pltpu.make_async_copy(acc, du.at[0], d_send.at[1]).start()
        logs = jnp.where(lax.axis_index("tp") == 0, jnp.sum(rows_ref[0, 2:3, :]), 0.0)
        own[0] = jnp.broadcast_to(logs - jnp.sum(found[...]), own.shape[1:])

    def finish():
        wait(acc, d_send.at[1])
        if N["tp"] > 1:
            wait(acc, d_send.at[0])
            wait(acc, d_recv)
        loss_ref[...] = own[len(AXES)] * hit_value

    pl.when(slot == 2 * dus)(finish_du)
    for i in range(len(AXES) + 1):
        pl.when(slot == 2 * (dus + i) + 1)(functools.partial(total, i, AXES, own, got, l_send, l_recv))
    pl.when(slot == pl.num_programs(0) - 1)(finish)


AXES = ("tp", "x", "y", "z")


def main_call(rows, u_all, ut_all, emb_t, logits):
    nx, ny, nz = N["x"], N["y"], N["z"]
    wg = nx * VB
    dus = VSH // DVB
    dma = pltpu.SemaphoreType.DMA

    def grad_block(s):
        return 0, lax.axis_index("z") * K + jnp.minimum(s // 2, K - 1)

    def du_block(s):
        return 0, jnp.minimum(s // 2, dus - 1)

    once = dict(pipeline_mode=pl.Buffered(1))
    return pl.pallas_call(
        main_kernel,
        grid=(2 * K + 12,),
        in_specs=[
            whole((nz, 8, T), **once),
            whole((nz * T, D), **once),
            whole((D, nz * T), **once),
            pl.BlockSpec((D, wg), grad_block),
            pl.BlockSpec((D, DVB), du_block),
            ANY,
        ],
        out_specs=[ANY, ANY, whole((8, LANES))],
        out_shape=[
            jax.ShapeDtypeStruct((ny, YR, VSH), F32),
            jax.ShapeDtypeStruct((2, T, DP), F32),
            jax.ShapeDtypeStruct((8, LANES), F32),
        ],
        scratch_shapes=[
            pltpu.VMEM(shape, F32)
            for shape in (
                (2, nz * T, LANES),
                (2, HALF, wg),
            )
        ]
        + [pltpu.VMEM((2, HALF, wg), BF16)]
        + [
            pltpu.VMEM(shape, F32)
            for shape in (
                (NP, nx, ny, YR, VB),
                (K, 2, 2, 2, RH, VB),
                (K, 2, 2, 4, RH, VB),
                (K, 2, RH, VB),
                (K, 2, 2, RH, VB),
                (NP, 2, 4, RH, VB),
                (K, YR, VB),
                (T, DVB),
                (T, DP),
            )
        ]
        + [
            pltpu.VMEM((2, T, SUB), BF16),
            pltpu.VMEM((T, LANES), F32),
            pltpu.VMEM((5, 8, LANES), F32),
            pltpu.VMEM((4, 3, 8, LANES), F32),
            dma((K, 2)),
            dma((K, 2, 4)),
            dma((K, len(COLORS))),
            dma((K, len(COLORS), 6)),
            dma((4, 3)),
            dma((4, 3)),
            dma((2,)),
            dma,
            dma,
            dma,
        ],
        compiler_params=params(collective_id=2, has_side_effects=True),
        cost_estimate=cost(6 * T * D * VSH, T * VSH * 4),
        name="main",
    )(rows, u_all, ut_all, emb_t, emb_t, logits)


def solution(mesh):
    axes = tuple(N)
    grid_mesh = Mesh(mesh.devices.reshape(tuple(N.values())), axes)

    def local_body(hidden, labels, loss_mask, norm_gain, embedding):
        emb_t = embedding.T
        hid_t = hidden.transpose(0, 2, 1)
        gain = norm_gain.astype(F32)[:, None]
        u, ut, pay = norm_call(hid_t, gain)
        logits, rows, ug = stats_call(pay, loss_mask, labels, u, emb_t)
        u_all, ut_all = pack_call(u, ut, ug)
        grad, du, loss = main_call(rows, u_all, ut_all, emb_t, logits)
        d_hidden = norm_back_call(hid_t, gain, du)
        return loss[0, 0], d_hidden.transpose(0, 2, 1), grad.reshape(D, VSH).T

    dp = axes[1:]
    return jax.shard_map(
        local_body,
        mesh=grid_mesh,
        in_specs=(P(dp), P(dp), P(dp), P(), P("tp")),
        out_specs=(P(), P(dp), P("tp")),
        check_vma=False,
    )
```
